512 devices in a mesh: ctx: 64 (over z, y), head: 2 (over core), pair: 4 (over x).
Axes of the slice: x: 4, y: 8, z: 8, core: 2. Of those that a mesh axis runs over, the one named last changes fastest.
Arguments:
- tokens_in: bfloat16 [2, 4096, 2048], P(None, ('ctx', 'pair')), may hold values from -6 to 6
- attn_gain: float32 [2048], replicated, may hold values from 0.1 to 1.9
- query_matrix: bfloat16 [2048, 2048], P(None, ('head', 'pair')), may hold values from -20 to 20
- key_matrix: bfloat16 [256, 2048], P(('head', 'pair')), may hold values from -1 to 1
- value_matrix: bfloat16 [256, 2048], P(('head', 'pair')), may hold values from -0.125 to 0.125
- output_matrix: bfloat16 [2048, 2048], P(None, ('head', 'pair')), may hold values from -0.125 to 0.125
- moe_gain: float32 [2048], replicated, may hold values from 0.1 to 1.9
- chosen_experts: int32 [2, 4096, 8], P('head', ('ctx', 'pair')), may hold values from 0 to 127, all different within a row; in each aligned block of 16 rows (0 to 15, 16 to 31, ..., all dimensions but the last counted through in order) at most 2 rows name the same one
- combine_weights: float32 [2, 4096, 8], P('head', ('ctx', 'pair')), may hold values from 0.02 to 0.5
- gate_weight: bfloat16 [128, 768, 2048], P(('ctx', 'head'), 'pair'), may hold values from -0.125 to 0.125
- up_weight: bfloat16 [128, 768, 2048], P(('ctx', 'head'), 'pair'), may hold values from -0.125 to 0.125
- down_weight: bfloat16 [128, 768, 2048], P(('ctx', 'head'), 'pair'), may hold values from -0.21875 to 0.21875
Outputs:
- layer_out: bfloat16 [2, 4096, 2048], P('head', ('ctx', 'pair'))
The draws below stay inside these ranges and needn't reach their ends.
Inputs may be any that keep to these rules, and one draw needn't show every extreme that they name: `chosen_experts`: each token names 8 different experts; among the 16 tokens of one sequence that one device holds, no expert is named more than 2 times.
All inputs are finite; a program needn't handle non-finite values.
Results may differ from the reference program's by a relative error of at most 0.013.
Values may be sent and summed in bfloat16 or wider, within the bound.
No kernel may reach another device: no remote copies, remote signals or barrier semaphores. Data moves between devices by JAX's collectives and lax.ppermute only.
A program may use at most 64 MiB of HBM per device.

```python
import math
import jax
import jax.numpy as jnp
import numpy as np
from jax import lax

MODEL_DIM = 2048
QUERY_HEADS = 16
KEY_VALUE_HEADS = 2
HEAD_SIZE = 128
FF = 768
TOP = 8
LEN_DEV = 16
SEQUENCE_COUNT = 2
SEQ_LENGTH = 4096
EXPERTS = 128
CAP = 2
N_PAIR = 4


def shared_key_rows(key):
    sampled_values = jax.random.normal(jax.random.fold_in(key, 17), (MODEL_DIM, KEY_VALUE_HEADS * HEAD_SIZE), jnp.float32)
    return jnp.clip(sampled_values, -6.0, 6.0) / jnp.sqrt(jnp.float32(MODEL_DIM))


def draw_key_matrix(key, part):
    return shared_key_rows(key).T.astype(jnp.bfloat16)


def draw_query_matrix(key, part):
    sampled_values = jax.random.normal(jax.random.fold_in(key, 29), (MODEL_DIM, QUERY_HEADS, HEAD_SIZE), jnp.float32)
    matrix_out = jnp.clip(sampled_values, -6.0, 6.0) / jnp.sqrt(jnp.float32(MODEL_DIM))
    return matrix_out.reshape(MODEL_DIM, QUERY_HEADS * HEAD_SIZE).astype(jnp.bfloat16)


def block_scale(stream_key, shape, split, smallest, top_value):
    def one(axis_at, parts):
        draws = jax.random.uniform(jax.random.fold_in(jax.random.fold_in(stream_key, 6), axis_at), (parts,), jnp.float32, smallest / len(split), top_value / len(split))
        return jnp.repeat(jnp.exp(draws), shape[axis_at] // parts).reshape((-1,) + (1,) * (len(shape) - axis_at - 1))

    level = one(*split[0])
    for cut in split[1:]:
        level = level * one(*cut)
    return level


def deal_out(own_key, own, number, rows, amount, top, most, skew):
    sequence = jax.random.permutation(own_key, amount)
    heavy_load, usual = load_shares(amount, rows * top, most, skew, True), load_shares(amount, rows * top, most, skew, False)
    places = jnp.arange(amount)

    def named(tallies, rotation):
        used = int((tallies > 0).sum())
        fixed = max(1, used // 4)
        passed = fixed + (places - fixed + rotation * (used - fixed)) % max(1, amount - fixed)
        return jnp.zeros((amount,), jnp.int32).at[sequence[jnp.where(places < fixed, places, passed)]].set(jnp.asarray(tallies, jnp.int32))

    tallies = jnp.where(number % 4 == 0, named(heavy_load, number // 4), named(usual, number - number // 4 - 1))
    mixed = jax.random.permutation(jax.random.fold_in(own, 3), amount)
    giver, taker = mixed[0:amount // 2 * 2:2], mixed[1:amount // 2 * 2:2]
    room = jnp.minimum(tallies[giver] - 1, most - tallies[taker]) // 2
    room = jnp.where((giver == sequence[0]) | (taker == sequence[0]) | (tallies[taker] == 0), 0, jnp.maximum(room, 0))
    passed = jax.random.randint(jax.random.fold_in(own, 4), (amount // 2,), 0, 1 << 20) % (room + 1)
    tallies = tallies.at[giver].add(-passed).at[taker].add(passed)
    items = jnp.searchsorted(jnp.cumsum(tallies), jnp.arange(rows * top), side="right").astype(jnp.int32)
    listing = items.reshape(top, rows).T
    listing = listing[jax.random.permutation(jax.random.fold_in(own, 1), rows)]
    rotation = jax.random.randint(jax.random.fold_in(own, 2), (rows, 1), 0, top)
    return jnp.take_along_axis(listing, (jnp.arange(top)[None, :] + rotation) % top, axis=1)


def load_shares(count, total, bound, skew, full):
    portions = [(1 << 20) // math.isqrt(grade ** skew) + 1 for grade in range(1, count + 1)]
    largest = bound if full else min(bound, max(-(-total // count), total * portions[0] // sum(portions)))
    least = 1 if total - largest >= count - 1 else 0
    counts, rest = [largest] + [least] * (count - 1), total - largest - least * (count - 1)
    while rest > 0:
        candidates = [i for i in range(1, count) if counts[i] < largest] or [i for i in range(1, count) if counts[i] < bound]
        whole, remaining = sum([portions[i] for i in candidates]), rest
        for i in candidates:
            more = min(bound - counts[i], max(1, remaining * portions[i] // whole), rest)
            counts[i] = counts[i] + more
            rest = rest - more
    return np.array(counts)


def noise(rng, extent, deviation, bound, pieces=(), dtype=jnp.bfloat16):
    entries = jax.random.normal(rng, extent, jnp.float32) * deviation
    if len(pieces) > 0:
        entries = block_scale(rng, extent, pieces, -0.22, 0.18) * entries
    return jnp.clip(entries, min=-bound, max=bound).astype(dtype)


def setup_inputs(seed: int = 0) -> dict:
    key_list = jax.random.split(jax.random.key(seed), 13)
    tokens_in = noise(key_list[0], (SEQUENCE_COUNT, SEQ_LENGTH, MODEL_DIM), 1.0, 6.0, ((1, 256),))
    attn_gain = jnp.clip(1.0 + 0.18 * jax.random.normal(key_list[1], (MODEL_DIM,), jnp.float32), 0.1, 1.9)
    query_matrix = draw_query_matrix(jax.random.fold_in(key_list[12], 71), 0)
    key_matrix = draw_key_matrix(jax.random.fold_in(key_list[12], 71), 0)
    value_matrix = noise(key_list[4], (KEY_VALUE_HEADS * HEAD_SIZE, MODEL_DIM), MODEL_DIM ** -0.5, 0.125, ((0, 8),))
    output_matrix = noise(key_list[5], (QUERY_HEADS * HEAD_SIZE, MODEL_DIM), (QUERY_HEADS * HEAD_SIZE) ** -0.5, 0.125, ((1, 8),))
    moe_gain = jnp.clip(1.0 + 0.18 * jax.random.normal(key_list[6], (MODEL_DIM,), jnp.float32), 0.1, 1.9)
    chosen_experts_keys = jax.random.split(jax.random.fold_in(key_list[7], 1), SEQUENCE_COUNT * SEQ_LENGTH // LEN_DEV)
    chosen_experts_turns = jax.random.permutation(jax.random.fold_in(key_list[7], 3), SEQUENCE_COUNT * SEQ_LENGTH // LEN_DEV)
    chosen_experts = jax.vmap(lambda own, number: deal_out(jax.random.fold_in(key_list[7], 2), own, number, LEN_DEV, EXPERTS, TOP, CAP, 0))(chosen_experts_keys, chosen_experts_turns).reshape((SEQUENCE_COUNT, SEQ_LENGTH, TOP))
    combine_weights = jnp.clip(jnp.exp(math.log(0.5) - 3.218876 * jax.random.uniform(key_list[8], (SEQUENCE_COUNT, SEQ_LENGTH, TOP), jnp.float32) ** block_scale(key_list[8], (SEQUENCE_COUNT, SEQ_LENGTH, TOP), ((0, 2), (1, 256)), -0.2, 0.2)), 0.02, 0.5)
    gate_weight = noise(key_list[9], (EXPERTS, FF, MODEL_DIM), MODEL_DIM ** -0.5, 0.125, ((0, 128), (1, 4)))
    up_weight = noise(key_list[10], (EXPERTS, FF, MODEL_DIM), MODEL_DIM ** -0.5, 0.125, ((0, 128), (1, 4)))
    down_weight = noise(key_list[11], (EXPERTS, FF, MODEL_DIM), FF ** -0.5, 0.21875, ((0, 128), (1, 4)))
    return dict(tokens_in=tokens_in, attn_gain=attn_gain, query_matrix=query_matrix, key_matrix=key_matrix, value_matrix=value_matrix, output_matrix=output_matrix, moe_gain=moe_gain, chosen_experts=chosen_experts, combine_weights=combine_weights, gate_weight=gate_weight, up_weight=up_weight, down_weight=down_weight)


ROPE_BASE = 1000000.0
EPSILON = 1e-06

def normalize(values, gain_vector):
    wide = values.astype(jnp.float32)
    mean_square = lax.optimization_barrier(jnp.mean(wide * wide, axis=-1, keepdims=True))
    return (wide * lax.rsqrt(mean_square + EPSILON) * gain_vector).astype(jnp.bfloat16)

def rotate(values, positions):
    half_dim = values.shape[-1] // 2
    frequency = ROPE_BASE ** (-(jnp.arange(half_dim).astype(jnp.float32) * 2.0) / values.shape[-1])
    angles = positions[:, None] * frequency[None, :]
    cosine_part = jnp.cos(angles)[:, None, :]
    sine_part = jnp.sin(angles)[:, None, :]
    lower_half = values[..., :half_dim]
    upper_half = values[..., half_dim:]
    return jnp.concatenate([lower_half * cosine_part - upper_half * sine_part, upper_half * cosine_part + lower_half * sine_part], axis=-1)

def reference(tokens_in, attn_gain, query_matrix, key_matrix, value_matrix, output_matrix, moe_gain, chosen_experts, combine_weights, gate_weight, up_weight, down_weight):
    normalized_input = normalize(tokens_in, attn_gain).astype(jnp.float32)
    positions = jnp.arange(SEQ_LENGTH).astype(jnp.float32)
    query_unrotated = jnp.einsum('ynx,xq->ynq', normalized_input, query_matrix.astype(jnp.float32)).reshape(SEQUENCE_COUNT, SEQ_LENGTH, QUERY_HEADS, HEAD_SIZE)
    queries = rotate(query_unrotated, positions).astype(jnp.bfloat16)
    key_unrotated = jnp.einsum('mzr,tr->mzt', normalized_input, key_matrix.astype(jnp.float32)).reshape(SEQUENCE_COUNT, SEQ_LENGTH, KEY_VALUE_HEADS, HEAD_SIZE)
    rotated_keys = rotate(key_unrotated, positions).astype(jnp.bfloat16)
    every_value_row = jnp.einsum('mzr,tr->mzt', normalized_input, value_matrix.astype(jnp.float32)).reshape(SEQUENCE_COUNT, SEQ_LENGTH, KEY_VALUE_HEADS, HEAD_SIZE).astype(jnp.bfloat16)
    group_width = QUERY_HEADS // KEY_VALUE_HEADS
    scaling = HEAD_SIZE ** (-0.5)
    causal = jnp.arange(SEQ_LENGTH)[None, :] <= jnp.arange(SEQ_LENGTH)[:, None]

    def attend(pair_id):
        seq_id = pair_id // QUERY_HEADS
        head_id = pair_id % QUERY_HEADS
        query_rows = queries[seq_id, :, head_id]
        key_rows = rotated_keys[seq_id, :, head_id // group_width]
        value_rows = every_value_row[seq_id, :, head_id // group_width]
        scores = jnp.dot(query_rows, key_rows.T, preferred_element_type=jnp.float32) * scaling
        scores = jnp.where(causal, scores, -1e+30)
        row_peak = lax.optimization_barrier(jnp.max(scores, axis=-1, keepdims=True))
        weights = jnp.where(causal, jnp.exp(scores - row_peak), 0.0)
        row_total = lax.optimization_barrier(jnp.sum(weights, axis=-1, keepdims=True))
        mixed = jnp.dot(weights.astype(jnp.bfloat16), value_rows, preferred_element_type=jnp.float32) / row_total
        return mixed.astype(jnp.bfloat16)
    head_results = lax.map(attend, jnp.arange(SEQUENCE_COUNT * QUERY_HEADS))
    head_results = head_results.reshape(SEQUENCE_COUNT, QUERY_HEADS, SEQ_LENGTH, HEAD_SIZE).transpose(0, 2, 1, 3).reshape(SEQUENCE_COUNT, SEQ_LENGTH, QUERY_HEADS * HEAD_SIZE)
    attention_output = jnp.einsum('kem,mv->kev', head_results.astype(jnp.float32), output_matrix.astype(jnp.float32)).astype(jnp.bfloat16)
    residual = (tokens_in.astype(jnp.float32) + attention_output.astype(jnp.float32)).astype(jnp.bfloat16)
    moe_in = normalize(residual, moe_gain).reshape(SEQUENCE_COUNT * SEQ_LENGTH, MODEL_DIM)
    flat_expert = chosen_experts.reshape(-1)
    flat_weight = combine_weights.reshape(-1)
    slot_count = CAP * (SEQUENCE_COUNT * SEQ_LENGTH // LEN_DEV)
    quarter = FF // N_PAIR

    def expert_step(totals, inputs):
        expert_id, gate_local, up_local, down_local = inputs
        matches = flat_expert == expert_id
        picked = jnp.nonzero(matches, size=slot_count, fill_value=0)[0].astype(jnp.int32)
        is_live = jnp.arange(slot_count) < jnp.sum(matches.astype(jnp.int32))
        token_ids = picked // TOP
        row_block = moe_in[token_ids]
        gate_part = lax.dot_general(row_block, gate_local, (((1,), (1,)), ((), ())), preferred_element_type=jnp.float32)
        up_part = lax.dot_general(row_block, up_local, (((1,), (1,)), ((), ())), preferred_element_type=jnp.float32)
        hidden = (jax.nn.silu(gate_part) * up_part).astype(jnp.bfloat16)
        output_sum = jnp.zeros((slot_count, MODEL_DIM), jnp.float32)
        for part_id in range(N_PAIR):
            lower_col = part_id * quarter
            partial_value = jnp.dot(hidden[:, lower_col:lower_col + quarter], down_local[lower_col:lower_col + quarter, :], preferred_element_type=jnp.float32)
            output_sum = output_sum + lax.optimization_barrier(partial_value.astype(jnp.bfloat16)).astype(jnp.float32)
        expert_out = lax.optimization_barrier(output_sum.astype(jnp.bfloat16)).astype(jnp.float32)
        scaled = jnp.where(is_live, flat_weight[picked], 0.0)[:, None] * expert_out
        return (totals.at[token_ids].add(scaled), None)
    totals, unused = lax.scan(expert_step, jnp.zeros((SEQUENCE_COUNT * SEQ_LENGTH, MODEL_DIM), jnp.float32), (jnp.arange(EXPERTS).astype(jnp.int32), gate_weight, up_weight, down_weight))
    mixture = totals.reshape(SEQUENCE_COUNT, SEQ_LENGTH, MODEL_DIM)
    return (residual.astype(jnp.float32) + mixture).astype(jnp.bfloat16)
```

```python
import jax
import jax.numpy as jnp
from jax import lax
from jax.sharding import PartitionSpec as P

ROPE_BASE = 1000000.0
EPSILON = 1e-06
MASKED = -1e30
F32 = jnp.float32
BF16 = jnp.bfloat16


def exchange(tiles, axis):
    return lax.all_to_all(tiles, axis, 0, 0, tiled=True)


def for_each(shard, count):
    return jnp.broadcast_to(shard[None], (count, *shard.shape))


def dot(a, b, a_dim, b_dim):
    return lax.dot_general(a, b, (((a_dim,), (b_dim,)), ((), ())), preferred_element_type=F32)


def normalize(values, gain_vector):
    wide = values.astype(F32)
    mean_square = jnp.mean(wide * wide, axis=-1, keepdims=True)
    return (wide * lax.rsqrt(mean_square + EPSILON) * gain_vector).astype(BF16)


def rope_tables(positions, head_dim):
    half_dim = head_dim // 2
    frequency = ROPE_BASE ** (-(jnp.arange(half_dim).astype(F32) * 2.0) / head_dim)
    angles = positions[:, None] * frequency[None, :]
    return jnp.cos(angles), jnp.sin(angles)


def rotate(values, tables):
    cosine_part, sine_part = tables
    half_dim = values.shape[-1] // 2
    lower_half = values[..., :half_dim]
    upper_half = values[..., half_dim:]
    return jnp.concatenate(
        [
            lower_half * cosine_part - upper_half * sine_part,
            upper_half * cosine_part + lower_half * sine_part,
        ],
        axis=-1,
    ).astype(BF16)


def rounded(values):
    return lax.reduce_precision(values, 8, 7)


def pieces(values):
    high = rounded(values)
    middle = rounded(values - high)
    return [high, middle, rounded(values - high - middle)]


def body(
    tokens_in,
    attn_gain,
    query_matrix,
    key_matrix,
    value_matrix,
    output_matrix,
    moe_gain,
    chosen_experts,
    combine_weights,
    gate_weight,
    up_weight,
    down_weight,
):
    pairs = lax.axis_size("pair")
    heads = lax.axis_size("head")
    blocks = lax.axis_size("ctx")
    seqs, own_len, width = tokens_in.shape
    own_rows = seqs * own_len
    rows = pairs * own_rows
    block_len = own_len * pairs
    q_cols = query_matrix.shape[1]
    part_cols = key_matrix.shape[0]
    head_dim = part_cols * pairs
    local_heads = q_cols // head_dim
    group = local_heads * pairs

    weights = lax.all_gather(
        jnp.concatenate([gate_weight[0], up_weight[0], down_weight[0]], axis=1),
        "pair",
        axis=0,
        tiled=True,
    )

    normed = normalize(tokens_in, attn_gain)
    block_rows = exchange(for_each(normed, pairs), "pair").reshape(rows, width)
    block_start = lax.axis_index("ctx") * block_len
    own_start = block_start + lax.axis_index("pair") * own_len
    places = jnp.arange(own_len)
    row_pos = block_start + (
        jnp.arange(pairs)[:, None, None] * own_len + jnp.zeros((seqs, 1), jnp.int32) + places
    ).reshape(rows)
    q_tables = rope_tables(row_pos.astype(F32), head_dim)
    key_value = dot(
        block_rows, jnp.concatenate([key_matrix, value_matrix], axis=0), 1, 1
    ).astype(BF16)
    query_raw = dot(block_rows, query_matrix, 1, 0)
    query = jnp.concatenate(
        [
            rotate(query_raw[:, j * head_dim : (j + 1) * head_dim], q_tables)
            for j in range(local_heads)
        ],
        axis=1,
    )
    swapped = exchange(
        jnp.concatenate(
            [
                for_each(query, pairs),
                jnp.pad(
                    key_value.reshape(pairs, own_rows, 2 * part_cols),
                    ((0, 0), (0, 0), (0, q_cols - 2 * part_cols)),
                ),
            ],
            axis=1,
        ),
        "pair",
    )
    own_pos = (own_start + jnp.zeros((seqs, 1), jnp.int32) + places).reshape(own_rows)
    key_own = jnp.concatenate([swapped[p, rows:, :part_cols] for p in range(pairs)], axis=1)
    value_own = jnp.concatenate(
        [swapped[p, rows:, part_cols : 2 * part_cols] for p in range(pairs)], axis=1
    )
    key_own = rotate(key_own.astype(F32), rope_tables(own_pos.astype(F32), head_dim))
    both = jnp.concatenate([key_own, value_own], axis=1)
    spread = exchange(for_each(both, blocks), "ctx").reshape(blocks, seqs, own_len, 2 * head_dim)
    spread = jnp.moveaxis(spread, 1, 0).reshape(seqs, blocks * own_len, 2 * head_dim)
    keys = spread[..., :head_dim]
    values = spread[..., head_dim:]

    queries = (
        swapped[:, :rows]
        .reshape(pairs, pairs, seqs, own_len, local_heads, head_dim)
        .transpose(2, 0, 4, 1, 3, 5)
        .reshape(seqs, group * block_len, head_dim)
    )
    key_pos = (
        jnp.arange(blocks)[:, None] * block_len + lax.axis_index("pair") * own_len + places
    ).reshape(1, blocks * own_len)
    query_pos = (jnp.zeros((group, 1), jnp.int32) + block_start + jnp.arange(block_len)).reshape(
        group * block_len, 1
    )
    allowed = (key_pos <= query_pos)[None]
    scores = jnp.einsum("sqd,skd->sqk", queries, keys, preferred_element_type=F32) * (
        head_dim ** (-0.5)
    )
    scores = jnp.where(allowed, scores, MASKED)
    peak = jnp.max(scores, axis=-1)
    probs = jnp.where(allowed, jnp.exp(scores - peak[..., None]), 0.0)
    total = jnp.sum(probs, axis=-1)
    mixed = jnp.einsum("sqk,skd->sqd", probs.astype(BF16), values, preferred_element_type=F32)

    stats = jnp.stack(pieces(peak) + pieces(total), axis=-1).astype(BF16)
    stats = stats.reshape(seqs, group, pairs, own_len, 6).transpose(2, 0, 3, 1, 4)
    stats = stats.reshape(pairs, own_rows, group * 6)
    mixed = (
        mixed.astype(BF16)
        .reshape(seqs, group, pairs, own_len, head_dim)
        .transpose(2, 0, 3, 1, 4)
        .reshape(pairs, own_rows, group * head_dim)
    )
    merged = exchange(
        jnp.concatenate(
            [mixed, jnp.pad(stats, ((0, 0), (0, 0), (0, head_dim - group * 6)))], axis=2
        ),
        "pair",
    )
    part_stats = (
        merged[..., group * head_dim : group * head_dim + group * 6]
        .astype(F32)
        .reshape(pairs, own_rows, group, 6)
    )
    part_peak = jnp.sum(part_stats[..., :3], axis=-1)
    part_total = jnp.sum(part_stats[..., 3:], axis=-1)
    scale = jnp.exp(part_peak - jnp.max(part_peak, axis=0))
    scale = scale / jnp.sum(scale * part_total, axis=0)
    part_mixed = merged[..., : group * head_dim].reshape(pairs, own_rows, group, head_dim)
    attended = jnp.sum(scale[..., None] * part_mixed.astype(F32), axis=0).astype(BF16)
    attended = attended.reshape(own_rows, group * head_dim)

    gathered_heads = exchange(for_each(attended, heads * pairs), ("head", "pair"))
    gathered_heads = gathered_heads.reshape(heads, rows, group * head_dim)
    projected = sum(
        dot(
            gathered_heads[h],
            output_matrix[h * group * head_dim : (h + 1) * group * head_dim],
            1,
            0,
        )
        for h in range(heads)
    ).astype(BF16)
    out_cols = output_matrix.shape[1]
    projected = (
        projected.reshape(pairs, seqs, own_len, out_cols)
        .transpose(1, 0, 2, 3)
        .reshape(seqs * pairs, own_len, out_cols)
    )
    owned = exchange(projected, ("head", "pair"))
    owned = jnp.moveaxis(owned, 0, 1).reshape(own_len, width)
    own_tokens = lax.dynamic_index_in_dim(tokens_in, lax.axis_index("head"), 0, keepdims=False)
    residual = (own_tokens.astype(F32) + owned.astype(F32)).astype(BF16)
    moe_in = normalize(residual, moe_gain)

    experts = blocks * heads
    top = chosen_experts.shape[-1]
    capacity = max(2, (own_len * top + experts - 1) // experts + 1)
    slots = experts * capacity
    picked = chosen_experts.reshape(own_len * top)
    earlier = jnp.tril(jnp.ones((own_len * top, own_len * top), jnp.bool_), -1)
    same = (picked[:, None] == picked[None, :]) & earlier
    slot_ids = picked * capacity + jnp.sum(same.astype(jnp.int32), axis=1)
    slot_ids = slot_ids.reshape(own_len, top)
    chosen_slot = slot_ids[..., None] == jnp.arange(slots)[None, None, :]
    placing = jnp.any(chosen_slot, axis=1).astype(BF16)
    outgoing = dot(placing, moe_in, 0, 0).astype(BF16)
    incoming = exchange(outgoing.reshape(experts, capacity, width), ("ctx", "head"))
    incoming = incoming.reshape(slots, width)
    gate_rows, up_rows, down_rows = jnp.split(weights, 3, axis=1)
    gate_part = dot(incoming, gate_rows, 1, 1)
    up_part = dot(incoming, up_rows, 1, 1)
    hidden = (jax.nn.silu(gate_part) * up_part).astype(BF16)
    expert_out = dot(hidden, down_rows, 1, 0).astype(BF16)
    returned = exchange(expert_out.reshape(experts, capacity, width), ("ctx", "head"))
    returned = returned.reshape(slots, width)
    gathered = returned[slot_ids.reshape(-1)].reshape(own_len, top, width)
    mixture = jnp.sum(
        combine_weights.reshape(own_len, top, 1) * gathered.astype(F32), axis=1
    )
    return (residual.astype(F32) + mixture).astype(BF16)[None]


def solution(mesh):
    return jax.shard_map(
        body,
        mesh=mesh,
        in_specs=(
            P(None, ("ctx", "pair"), None),
            P(),
            P(None, ("head", "pair")),
            P(("head", "pair"), None),
            P(("head", "pair"), None),
            P(None, ("head", "pair")),
            P(),
            P("head", ("ctx", "pair"), None),
            P("head", ("ctx", "pair"), None),
            P(("ctx", "head"), "pair", None),
            P(("ctx", "head"), "pair", None),
            P(("ctx", "head"), "pair", None),
        ),
        out_specs=P("head", ("ctx", "pair"), None),
        check_vma=False,
    )
```

```python
import jax
import jax.numpy as jnp
from jax import lax
from jax.experimental import pallas as pl
from jax.experimental.pallas import tpu as pltpu
from jax.sharding import PartitionSpec as P


ROPE_BASE = 1000000.0
EPSILON = 1e-06
MASKED = -1e30
F32 = jnp.float32
BF16 = jnp.bfloat16


def exchange(tiles, axis):
    return lax.all_to_all(tiles, axis, 0, 0, tiled=True)


def for_each(shard, count):
    return jnp.broadcast_to(shard[None], (count, *shard.shape))


def dot(a, b, a_dim, b_dim):
    return lax.dot_general(a, b, (((a_dim,), (b_dim,)), ((), ())), preferred_element_type=F32)


def normalize(values, gain_vector):
    wide = values.astype(F32)
    mean_square = jnp.mean(wide * wide, axis=-1, keepdims=True)
    return (wide * lax.rsqrt(mean_square + EPSILON) * gain_vector).astype(BF16)


def rope_tables(positions, head_dim):
    half_dim = head_dim // 2
    frequency = ROPE_BASE ** (-(jnp.arange(half_dim).astype(F32) * 2.0) / head_dim)
    angles = positions[:, None] * frequency[None, :]
    return jnp.cos(angles), jnp.sin(angles)


def rotate(values, tables):
    cosine_part, sine_part = tables
    half_dim = values.shape[-1] // 2
    lower_half = values[..., :half_dim]
    upper_half = values[..., half_dim:]
    return jnp.concatenate(
        [
            lower_half * cosine_part - upper_half * sine_part,
            upper_half * cosine_part + lower_half * sine_part,
        ],
        axis=-1,
    ).astype(BF16)


STATS = 6


def attend_part(where, query_slots, spread, seqs, own_len, block_len, local_heads, head_dim):
    pairs = len(query_slots)
    own_rows = seqs * own_len
    blocks = spread.shape[0]
    lanes = pairs * local_heads * head_dim
    scaling = head_dim ** (-0.5)

    def kernel(where_ref, *refs):
        query_refs = refs[:pairs]
        spread_ref, out_ref = refs[pairs:]
        start = where_ref[0]
        me = where_ref[1]
        key_shape = (own_len, blocks * own_len)
        key_index = lax.broadcasted_iota(jnp.int32, key_shape, 1)
        place = lax.broadcasted_iota(jnp.int32, key_shape, 0)
        lag = (
            (key_index // own_len) * block_len + me * own_len + key_index % own_len - place
        )
        lane = lax.broadcasted_iota(jnp.int32, (own_len, head_dim), 1)
        for seq in range(seqs):
            low = seq * own_len
            keys = spread_ref[:, low : low + own_len, :head_dim].reshape(-1, head_dim)
            values = spread_ref[:, low : low + own_len, head_dim:].reshape(-1, head_dim)
            stats = {}
            for t in range(pairs):
                owners = [lax.rem(me - t - s + 2 * pairs, pairs) for s in range(pairs)]
                allowed = jnp.concatenate([lag <= start + o * own_len for o in owners], axis=0)
                for j in range(local_heads):
                    head = t * local_heads + j
                    query = jnp.concatenate(
                        [
                            query_refs[t][
                                s, low : low + own_len, j * head_dim : (j + 1) * head_dim
                            ]
                            for s in range(pairs)
                        ],
                        axis=0,
                    )
                    scores = dot(query, keys, 1, 1) * scaling
                    scores = jnp.where(allowed, scores, MASKED)
                    peak = jnp.max(scores, axis=1, keepdims=True)
                    probs = jnp.where(allowed, jnp.exp(scores - peak), 0.0)
                    total = jnp.sum(probs, axis=1, keepdims=True)
                    mixed = dot(probs.astype(BF16), values, 1, 0).astype(BF16)
                    terms = []
                    for number in (peak, total):
                        high = number.astype(BF16).astype(F32)
                        middle = (number - high).astype(BF16).astype(F32)
                        terms += [high, middle, number - high - middle]
                    for s in range(pairs):
                        span = slice(s * own_len, (s + 1) * own_len)
                        out_ref[
                            owners[s],
                            low : low + own_len,
                            head * head_dim : (head + 1) * head_dim,
                        ] = mixed[span]
                        at = (t + s) % pairs
                        row = stats.get(at, jnp.zeros((own_len, head_dim), F32))
                        for n, term in enumerate(terms):
                            row = jnp.where(lane == head * STATS + n, term[span], row)
                        stats[at] = row
            for at in range(pairs):
                out_ref[lax.rem(me - at + pairs, pairs), low : low + own_len, lanes:] = stats[
                    at
                ].astype(BF16)

    vmem = pl.BlockSpec(memory_space=pltpu.VMEM)
    return pl.pallas_call(
        kernel,
        out_shape=jax.ShapeDtypeStruct((pairs, own_rows, lanes + head_dim), BF16),
        in_specs=[pl.BlockSpec(memory_space=pltpu.SMEM)] + [vmem] * (pairs + 1),
        out_specs=vmem,
        name="attend_part",
    )(where, *query_slots, spread)


def merge_parts(merged, own_rows, local_heads, head_dim):
    pairs = merged.shape[0]
    lanes = pairs * local_heads * head_dim

    def kernel(in_ref, out_ref):
        stats = [in_ref[p, :, lanes:].astype(F32) for p in range(pairs)]
        for g in range(pairs):
            for j in range(local_heads):
                heads = [((p - g) % pairs) * local_heads + j for p in range(pairs)]

                def number(p, first):
                    at = heads[p] * STATS + first
                    return (
                        stats[p][:, at : at + 1]
                        + stats[p][:, at + 1 : at + 2]
                        + stats[p][:, at + 2 : at + 3]
                    )

                peaks = [number(p, 0) for p in range(pairs)]
                top = peaks[0]
                for peak in peaks[1:]:
                    top = jnp.maximum(top, peak)
                scales = [jnp.exp(peak - top) for peak in peaks]
                total = sum(scales[p] * number(p, 3) for p in range(pairs))
                mix = sum(
                    scales[p]
                    * in_ref[p, :, heads[p] * head_dim : (heads[p] + 1) * head_dim].astype(F32)
                    for p in range(pairs)
                )
                head = g * local_heads + j
                out_ref[:, head * head_dim : (head + 1) * head_dim] = (mix / total).astype(BF16)

    vmem = pl.BlockSpec(memory_space=pltpu.VMEM)
    return pl.pallas_call(
        kernel,
        out_shape=jax.ShapeDtypeStruct((own_rows, lanes), BF16),
        in_specs=[vmem],
        out_specs=vmem,
        name="merge_parts",
    )(merged)


def body(
    tokens_in,
    attn_gain,
    query_matrix,
    key_matrix,
    value_matrix,
    output_matrix,
    moe_gain,
    chosen_experts,
    combine_weights,
    gate_weight,
    up_weight,
    down_weight,
):
    pairs = lax.axis_size("pair")
    heads = lax.axis_size("head")
    blocks = lax.axis_size("ctx")
    seqs, own_len, width = tokens_in.shape
    own_rows = seqs * own_len
    rows = pairs * own_rows
    block_len = own_len * pairs
    q_cols = query_matrix.shape[1]
    part_cols = key_matrix.shape[0]
    head_dim = part_cols * pairs
    local_heads = q_cols // head_dim
    group = local_heads * pairs

    places = jnp.arange(own_len)
    block_start = lax.axis_index("ctx") * block_len
    me = lax.axis_index("pair")
    own_pos = (block_start + me * own_len + jnp.zeros((seqs, 1), jnp.int32) + places).reshape(
        own_rows
    )
    own_tables = rope_tables(own_pos.astype(F32), head_dim)
    normed = normalize(tokens_in, attn_gain).reshape(own_rows, width)
    kv_send = for_each(jnp.concatenate([key_matrix, value_matrix], axis=0), pairs)
    kv_rows = exchange(kv_send, "pair")

    joined = jnp.concatenate([gate_weight[0], up_weight[0], down_weight[0]], axis=1)
    weights = lax.all_gather(joined, "pair", axis=0, tiled=True)
    key_own = dot(normed, kv_rows[:, :part_cols].reshape(head_dim, width), 1, 1)
    value_own = dot(normed, kv_rows[:, part_cols:].reshape(head_dim, width), 1, 1)
    both = jnp.concatenate([rotate(key_own, own_tables), value_own.astype(BF16)], axis=1)
    to_send = for_each(both, blocks)
    spread = exchange(to_send, "ctx")

    normed, _ = lax.optimization_barrier((normed, to_send))

    def from_below(shard):
        return [shard] + [
            lax.ppermute(shard, "pair", [(i, (i + t) % pairs) for i in range(pairs)])
            for t in range(1, pairs)
        ]

    token_slots = jnp.concatenate(from_below(normed), axis=0)
    slot_pair = (me - jnp.arange(pairs)) % pairs
    row_pos = (
        block_start
        + slot_pair[:, None, None] * own_len
        + jnp.zeros((seqs, 1), jnp.int32)
        + places
    ).reshape(rows)
    q_tables = rope_tables(row_pos.astype(F32), head_dim)
    query_raw = dot(token_slots, query_matrix, 1, 0)
    query = jnp.concatenate(
        [
            rotate(query_raw[:, j * head_dim : (j + 1) * head_dim], q_tables)
            for j in range(local_heads)
        ],
        axis=1,
    )
    query_slots = [q.reshape(pairs, own_rows, q_cols) for q in from_below(query)]
    parts = attend_part(
        jnp.stack([block_start, me]).astype(jnp.int32),
        query_slots,
        spread,
        seqs,
        own_len,
        block_len,
        local_heads,
        head_dim,
    )
    merged = exchange(parts, "pair")
    attended = merge_parts(merged, own_rows, local_heads, head_dim)

    gathered_heads = exchange(for_each(attended, heads * pairs), ("head", "pair"))
    gathered_heads = gathered_heads.reshape(heads, rows, group * head_dim)
    projected = sum(
        dot(
            gathered_heads[h],
            output_matrix[h * group * head_dim : (h + 1) * group * head_dim],
            1,
            0,
        )
        for h in range(heads)
    ).astype(BF16)
    out_cols = output_matrix.shape[1]
    projected = (
        projected.reshape(pairs, seqs, own_len, out_cols)
        .transpose(1, 0, 2, 3)
        .reshape(seqs * pairs, own_len, out_cols)
    )
    owned = exchange(projected, ("head", "pair"))
    owned = jnp.moveaxis(owned, 0, 1).reshape(own_len, width)
    own_tokens = lax.dynamic_index_in_dim(tokens_in, lax.axis_index("head"), 0, keepdims=False)
    residual = (own_tokens.astype(F32) + owned.astype(F32)).astype(BF16)
    moe_in = normalize(residual, moe_gain)

    experts = blocks * heads
    top = chosen_experts.shape[-1]
    capacity = max(2, (own_len * top + experts - 1) // experts + 1)
    slots = experts * capacity
    picked = chosen_experts.reshape(own_len * top)
    earlier = jnp.tril(jnp.ones((own_len * top, own_len * top), jnp.bool_), -1)
    same = (picked[:, None] == picked[None, :]) & earlier
    slot_ids = picked * capacity + jnp.sum(same.astype(jnp.int32), axis=1)
    slot_ids = slot_ids.reshape(own_len, top)
    chosen_slot = slot_ids[..., None] == jnp.arange(slots)[None, None, :]
    placing = jnp.any(chosen_slot, axis=1).astype(BF16)
    outgoing = dot(placing, moe_in, 0, 0).astype(BF16)
    incoming = exchange(outgoing.reshape(experts, capacity, width), ("ctx", "head"))
    incoming = incoming.reshape(slots, width)
    gate_rows, up_rows, down_rows = jnp.split(weights, 3, axis=1)
    gate_part = dot(incoming, gate_rows, 1, 1)
    up_part = dot(incoming, up_rows, 1, 1)
    hidden = (jax.nn.silu(gate_part) * up_part).astype(BF16)
    expert_out = dot(hidden, down_rows, 1, 0).astype(BF16)
    returned = exchange(expert_out.reshape(experts, capacity, width), ("ctx", "head"))
    returned = returned.reshape(slots, width)
    gathered = returned[slot_ids.reshape(-1)].reshape(own_len, top, width)
    mixture = jnp.sum(
        combine_weights.reshape(own_len, top, 1) * gathered.astype(F32), axis=1
    )
    return (residual.astype(F32) + mixture).astype(BF16)[None]


def solution(mesh):
    return jax.shard_map(
        body,
        mesh=mesh,
        in_specs=(
            P(None, ("ctx", "pair"), None),
            P(),
            P(None, ("head", "pair")),
            P(("head", "pair"), None),
            P(("head", "pair"), None),
            P(None, ("head", "pair")),
            P(),
            P("head", ("ctx", "pair"), None),
            P("head", ("ctx", "pair"), None),
            P(("ctx", "head"), "pair", None),
            P(("ctx", "head"), "pair", None),
            P(("ctx", "head"), "pair", None),
        ),
        out_specs=P("head", ("ctx", "pair"), None),
        check_vma=False,
    )
```

```python
import jax
import jax.numpy as jnp
from jax import lax
from jax.experimental import pallas as pl
from jax.experimental.pallas import tpu as pltpu
from jax.sharding import PartitionSpec as P


ROPE_BASE = 1000000.0
EPSILON = 1e-06
MASKED = -1e30
F32 = jnp.float32
BF16 = jnp.bfloat16


def exchange(tiles, axis):
    return lax.all_to_all(tiles, axis, 0, 0, tiled=True)


def for_each(shard, count):
    return jnp.broadcast_to(shard[None], (count, *shard.shape))


def dot(a, b, a_dim, b_dim):
    return lax.dot_general(a, b, (((a_dim,), (b_dim,)), ((), ())), preferred_element_type=F32)


def normalize(values, gain_vector):
    wide = values.astype(F32)
    mean_square = jnp.mean(wide * wide, axis=-1, keepdims=True)
    return (wide * lax.rsqrt(mean_square + EPSILON) * gain_vector).astype(BF16)


def rope_tables(positions, head_dim):
    half_dim = head_dim // 2
    frequency = ROPE_BASE ** (-(jnp.arange(half_dim).astype(F32) * 2.0) / head_dim)
    angles = positions[:, None] * frequency[None, :]
    return jnp.cos(angles), jnp.sin(angles)


def rotate(values, tables):
    cosine_part, sine_part = tables
    half_dim = values.shape[-1] // 2
    lower_half = values[..., :half_dim]
    upper_half = values[..., half_dim:]
    return jnp.concatenate(
        [
            lower_half * cosine_part - upper_half * sine_part,
            upper_half * cosine_part + lower_half * sine_part,
        ],
        axis=-1,
    ).astype(BF16)


def rounded(values):
    return lax.reduce_precision(values, 8, 7)


STATS = 6
LOG2_E = 1.4426950408889634
GROUP_ROWS = 256


def attend_part(where, swapped, spread, seqs, own_len, local_heads, head_dim):
    pairs = swapped.shape[0]
    own_rows = seqs * own_len
    block_len = pairs * own_len
    blocks = spread.shape[0]
    group = pairs * local_heads
    lanes = group * head_dim
    scaling = head_dim ** (-0.5)
    heads_each = GROUP_ROWS // block_len

    def kernel(where_ref, swapped_ref, spread_ref, out_ref):
        start = where_ref[0]
        me = where_ref[1]
        key_index = lax.broadcasted_iota(jnp.int32, (1, blocks * own_len), 1)
        key_pos = (key_index // own_len) * block_len + me * own_len + key_index % own_len
        row = lax.broadcasted_iota(jnp.int32, (GROUP_ROWS, 1), 0)
        allowed = key_pos <= start + row % block_len
        lane = lax.broadcasted_iota(jnp.int32, (block_len, head_dim), 1)
        for seq in range(seqs):
            low = seq * own_len
            keys = spread_ref[:, low : low + own_len, :head_dim].reshape(-1, head_dim)
            values = spread_ref[:, low : low + own_len, head_dim:].reshape(-1, head_dim)
            stats = jnp.zeros((block_len, head_dim), F32)
            for first in range(0, group, heads_each):
                query = jnp.concatenate(
                    [
                        swapped_ref[
                            g // local_heads,
                            p * own_rows + low : p * own_rows + low + own_len,
                            (g % local_heads) * head_dim : (g % local_heads + 1) * head_dim,
                        ]
                        for g in range(first, first + heads_each)
                        for p in range(pairs)
                    ],
                    axis=0,
                )
                scores = jnp.where(allowed, dot(query, keys, 1, 1), MASKED)
                peak = jnp.maximum(jnp.max(scores, axis=1, keepdims=True), 0.1 * MASKED)
                probs = jnp.exp2((scores - peak) * (scaling * LOG2_E))
                total = jnp.sum(probs, axis=1, keepdims=True)
                mixed = dot(probs.astype(BF16), values, 1, 0).astype(BF16)
                terms = []
                for number in (peak * scaling, total):
                    high = number.astype(BF16).astype(F32)
                    middle = (number - high).astype(BF16).astype(F32)
                    terms += [high, middle, number - high - middle]
                for g in range(first, first + heads_each):
                    top = (g - first) * block_len
                    for p in range(pairs):
                        at = top + p * own_len
                        out_ref[
                            p, low : low + own_len, g * head_dim : (g + 1) * head_dim
                        ] = mixed[at : at + own_len]
                    for n, term in enumerate(terms):
                        stats = jnp.where(
                            lane == g * STATS + n, term[top : top + block_len], stats
                        )
            for p in range(pairs):
                out_ref[p, low : low + own_len, lanes:] = stats[
                    p * own_len : (p + 1) * own_len
                ].astype(BF16)

    vmem = pl.BlockSpec(memory_space=pltpu.VMEM)
    return pl.pallas_call(
        kernel,
        out_shape=jax.ShapeDtypeStruct((pairs, own_rows, lanes + head_dim), BF16),
        in_specs=[pl.BlockSpec(memory_space=pltpu.SMEM), vmem, vmem],
        out_specs=vmem,
        name="attend_part",
    )(where, swapped, spread)


def experts_forward(incoming, weights):
    slots, width = incoming.shape
    hidden_units = weights.shape[0]
    step_units = 256 if hidden_units % 256 == 0 else hidden_units

    def kernel(rows_ref, gate_ref, up_ref, down_ref, out_ref, sum_ref):
        step = pl.program_id(0)
        gate_part = dot(rows_ref[...], gate_ref[...], 1, 1)
        up_part = dot(rows_ref[...], up_ref[...], 1, 1)
        hidden = (gate_part / (1.0 + jnp.exp(-gate_part)) * up_part).astype(BF16)
        part = dot(hidden, down_ref[...], 1, 0)

        @pl.when(step == 0)
        def _():
            sum_ref[...] = part

        @pl.when(step > 0)
        def _():
            sum_ref[...] += part

        @pl.when(step == pl.num_programs(0) - 1)
        def _():
            out_ref[...] = sum_ref[...].astype(BF16)

    whole = pl.BlockSpec((slots, width), lambda i: (0, 0))
    return pl.pallas_call(
        kernel,
        grid=(hidden_units // step_units,),
        out_shape=jax.ShapeDtypeStruct((slots, width), BF16),
        in_specs=[
            whole,
            pl.BlockSpec((step_units, width), lambda i: (i, 0)),
            pl.BlockSpec((step_units, width), lambda i: (i, 1)),
            pl.BlockSpec((step_units, width), lambda i: (i, 2)),
        ],
        out_specs=whole,
        scratch_shapes=[pltpu.VMEM((slots, width), F32)],
        compiler_params=pltpu.CompilerParams(dimension_semantics=("arbitrary",)),
        name="experts_forward",
    )(incoming, weights, weights, weights)


def body(
    tokens_in,
    attn_gain,
    query_matrix,
    key_matrix,
    value_matrix,
    output_matrix,
    moe_gain,
    chosen_experts,
    combine_weights,
    gate_weight,
    up_weight,
    down_weight,
):
    pairs = lax.axis_size("pair")
    heads = lax.axis_size("head")
    blocks = lax.axis_size("ctx")
    seqs, own_len, width = tokens_in.shape
    own_rows = seqs * own_len
    rows = pairs * own_rows
    block_len = own_len * pairs
    q_cols = query_matrix.shape[1]
    part_cols = key_matrix.shape[0]
    head_dim = part_cols * pairs
    local_heads = q_cols // head_dim
    group = local_heads * pairs

    joined = jnp.concatenate([gate_weight[0], up_weight[0], down_weight[0]], axis=1)
    weights = lax.all_gather(joined, "pair", axis=0, tiled=True)

    normed = normalize(tokens_in, attn_gain)
    token_send = for_each(normed, pairs)
    block_rows = exchange(token_send, "pair").reshape(rows, width)
    block_start = lax.axis_index("ctx") * block_len
    own_start = block_start + lax.axis_index("pair") * own_len
    places = jnp.arange(own_len)
    row_pos = block_start + (
        jnp.arange(pairs)[:, None, None] * own_len + jnp.zeros((seqs, 1), jnp.int32) + places
    ).reshape(rows)
    q_tables = rope_tables(row_pos.astype(F32), head_dim)
    key_value = dot(
        block_rows, jnp.concatenate([key_matrix, value_matrix], axis=0), 1, 1
    ).astype(BF16)
    query_raw = dot(block_rows, query_matrix, 1, 0)
    query = jnp.concatenate(
        [
            rotate(query_raw[:, j * head_dim : (j + 1) * head_dim], q_tables)
            for j in range(local_heads)
        ],
        axis=1,
    )
    swapped = exchange(
        jnp.concatenate(
            [
                for_each(query, pairs),
                jnp.pad(
                    key_value.reshape(pairs, own_rows, 2 * part_cols),
                    ((0, 0), (0, 0), (0, q_cols - 2 * part_cols)),
                ),
            ],
            axis=1,
        ),
        "pair",
    )
    own_pos = (own_start + jnp.zeros((seqs, 1), jnp.int32) + places).reshape(own_rows)
    key_own = jnp.concatenate([swapped[p, rows:, :part_cols] for p in range(pairs)], axis=1)
    value_own = jnp.concatenate(
        [swapped[p, rows:, part_cols : 2 * part_cols] for p in range(pairs)], axis=1
    )
    key_own = rotate(key_own.astype(F32), rope_tables(own_pos.astype(F32), head_dim))
    both = jnp.concatenate([key_own, value_own], axis=1)
    kv_send = for_each(both, blocks)
    spread = exchange(kv_send, "ctx")

    head = lax.axis_index("head")
    group_cols = group * head_dim
    out_mine = lax.dynamic_slice_in_dim(output_matrix, head * group_cols, group_cols, 0)
    out_theirs = lax.dynamic_slice_in_dim(
        output_matrix, (heads - 1 - head) * group_cols, group_cols, 0
    )
    out_other = lax.ppermute(
        out_theirs, "head", [(h, heads - 1 - h) for h in range(heads)]
    )

    parts = attend_part(
        jnp.stack([block_start, lax.axis_index("pair")]).astype(jnp.int32),
        swapped,
        spread,
        seqs,
        own_len,
        local_heads,
        head_dim,
    )
    merged = exchange(parts, "pair")
    part_stats = (
        merged[..., group * head_dim : group * head_dim + group * 6]
        .astype(F32)
        .reshape(pairs, own_rows, group, 6)
    )
    part_peak = jnp.sum(part_stats[..., :3], axis=-1)
    part_total = jnp.sum(part_stats[..., 3:], axis=-1)
    scale = jnp.exp(part_peak - jnp.max(part_peak, axis=0))
    scale = scale / jnp.sum(scale * part_total, axis=0)
    part_mixed = merged[..., : group * head_dim].reshape(pairs, own_rows, group, head_dim)
    attended = jnp.sum(scale[..., None] * part_mixed.astype(F32), axis=0).astype(BF16)
    attended = attended.reshape(own_rows, group * head_dim)

    gathered_heads = exchange(for_each(attended, pairs), "pair").reshape(rows, group_cols)
    projected = jnp.stack(
        [dot(gathered_heads, out_mine, 1, 0), dot(gathered_heads, out_other, 1, 0)]
    ).astype(BF16)
    out_cols = output_matrix.shape[1]
    projected = (
        projected.reshape(2, pairs, seqs, own_len, out_cols)
        .transpose(2, 1, 0, 3, 4)
        .reshape(seqs * pairs, 2 * own_len, out_cols)
    )
    owned = exchange(projected, ("head", "pair")).reshape(
        heads, pairs, 2, own_len, out_cols
    ).astype(F32)
    owned = (owned[:, :, 0] + owned[::-1, :, 1]).reshape(heads * pairs, own_len, out_cols)
    owned = jnp.moveaxis(owned, 0, 1).reshape(own_len, width)
    own_tokens = lax.dynamic_index_in_dim(tokens_in, lax.axis_index("head"), 0, keepdims=False)
    residual = (own_tokens.astype(F32) + rounded(owned)).astype(BF16)
    moe_in = normalize(residual, moe_gain)

    experts = blocks * heads
    top = chosen_experts.shape[-1]
    capacity = max(2, (own_len * top + experts - 1) // experts + 1)
    slots = experts * capacity
    picked = chosen_experts.reshape(own_len * top)
    earlier = jnp.tril(jnp.ones((own_len * top, own_len * top), jnp.bool_), -1)
    same = (picked[:, None] == picked[None, :]) & earlier
    slot_ids = picked * capacity + jnp.sum(same.astype(jnp.int32), axis=1)
    slot_ids = slot_ids.reshape(own_len, top)
    chosen_slot = slot_ids[..., None] == jnp.arange(slots)[None, None, :]
    placing = jnp.any(chosen_slot, axis=1).astype(BF16)
    outgoing = dot(placing, moe_in, 0, 0).astype(BF16)
    incoming = exchange(outgoing.reshape(experts, capacity, width), ("ctx", "head"))
    incoming = incoming.reshape(slots, width)
    expert_out = experts_forward(incoming, weights)
    returned = exchange(expert_out.reshape(experts, capacity, width), ("ctx", "head"))
    returned = returned.reshape(slots, width)
    share = jnp.sum(
        jnp.where(chosen_slot, combine_weights.reshape(own_len, top, 1), 0.0), axis=1
    )
    high = rounded(share)
    mixture = dot(jnp.concatenate([high, share - high], axis=0).astype(BF16), returned, 1, 0)
    mixture = mixture[:own_len] + mixture[own_len:]
    return (residual.astype(F32) + mixture).astype(BF16)[None]


def solution(mesh):
    return jax.shard_map(
        body,
        mesh=mesh,
        in_specs=(
            P(None, ("ctx", "pair"), None),
            P(),
            P(None, ("head", "pair")),
            P(("head", "pair"), None),
            P(("head", "pair"), None),
            P(None, ("head", "pair")),
            P(),
            P("head", ("ctx", "pair"), None),
            P("head", ("ctx", "pair"), None),
            P(("ctx", "head"), "pair", None),
            P(("ctx", "head"), "pair", None),
            P(("ctx", "head"), "pair", None),
        ),
        out_specs=P("head", ("ctx", "pair"), None),
        check_vma=False,
    )
```

```python
import jax
import jax.numpy as jnp
from jax import lax
from jax.experimental import pallas as pl
from jax.experimental.pallas import tpu as pltpu
from jax.sharding import PartitionSpec as P


ROPE_BASE = 1000000.0
EPSILON = 1e-06
MASKED = -1e30
F32 = jnp.float32
BF16 = jnp.bfloat16


def exchange(tiles, axis):
    return lax.all_to_all(tiles, axis, 0, 0, tiled=True)


def for_each(shard, count):
    return jnp.broadcast_to(shard[None], (count, *shard.shape))


def dot(a, b, a_dim, b_dim):
    return lax.dot_general(a, b, (((a_dim,), (b_dim,)), ((), ())), preferred_element_type=F32)


def normalize(values, gain_vector):
    wide = values.astype(F32)
    mean_square = jnp.mean(wide * wide, axis=-1, keepdims=True)
    return (wide * lax.rsqrt(mean_square + EPSILON) * gain_vector).astype(BF16)


def rope_tables(positions, head_dim):
    half_dim = head_dim // 2
    frequency = ROPE_BASE ** (-(jnp.arange(half_dim).astype(F32) * 2.0) / head_dim)
    angles = positions[:, None] * frequency[None, :]
    return jnp.cos(angles), jnp.sin(angles)


def rotate(values, tables):
    cosine_part, sine_part = tables
    half_dim = values.shape[-1] // 2
    lower_half = values[..., :half_dim]
    upper_half = values[..., half_dim:]
    return jnp.concatenate(
        [
            lower_half * cosine_part - upper_half * sine_part,
            upper_half * cosine_part + lower_half * sine_part,
        ],
        axis=-1,
    ).astype(BF16)


def rounded(values):
    return lax.reduce_precision(values, 8, 7)


STATS = 6
LOG2_E = 1.4426950408889634
GROUP_ROWS = 256


def attend_part(where, swapped, spread, seqs, own_len, local_heads, head_dim):
    pairs = swapped.shape[0]
    own_rows = seqs * own_len
    block_len = pairs * own_len
    blocks = spread.shape[0]
    group = pairs * local_heads
    lanes = group * head_dim
    scaling = head_dim ** (-0.5)
    heads_each = GROUP_ROWS // block_len

    def kernel(where_ref, swapped_ref, spread_ref, out_ref):
        start = where_ref[0]
        me = where_ref[1]
        key_index = lax.broadcasted_iota(jnp.int32, (1, blocks * own_len), 1)
        key_pos = (key_index // own_len) * block_len + me * own_len + key_index % own_len
        row = lax.broadcasted_iota(jnp.int32, (GROUP_ROWS, 1), 0)
        allowed = key_pos <= start + row % block_len
        lane = lax.broadcasted_iota(jnp.int32, (block_len, head_dim), 1)
        for seq in range(seqs):
            low = seq * own_len
            keys = spread_ref[:, low : low + own_len, :head_dim].reshape(-1, head_dim)
            values = spread_ref[:, low : low + own_len, head_dim:].reshape(-1, head_dim)
            stats = jnp.zeros((block_len, head_dim), F32)
            for first in range(0, group, heads_each):
                query = jnp.concatenate(
                    [
                        swapped_ref[
                            g // local_heads,
                            p * own_rows + low : p * own_rows + low + own_len,
                            (g % local_heads) * head_dim : (g % local_heads + 1) * head_dim,
                        ]
                        for g in range(first, first + heads_each)
                        for p in range(pairs)
                    ],
                    axis=0,
                )
                scores = jnp.where(allowed, dot(query, keys, 1, 1), MASKED)
                peak = jnp.maximum(jnp.max(scores, axis=1, keepdims=True), 0.1 * MASKED)
                probs = jnp.exp2((scores - peak) * (scaling * LOG2_E))
                total = jnp.sum(probs, axis=1, keepdims=True)
                mixed = dot(probs.astype(BF16), values, 1, 0).astype(BF16)
                terms = []
                for number in (peak * scaling, total):
                    high = number.astype(BF16).astype(F32)
                    middle = (number - high).astype(BF16).astype(F32)
                    terms += [high, middle, number - high - middle]
                for g in range(first, first + heads_each):
                    top = (g - first) * block_len
                    for p in range(pairs):
                        at = top + p * own_len
                        out_ref[
                            p, low : low + own_len, g * head_dim : (g + 1) * head_dim
                        ] = mixed[at : at + own_len]
                    for n, term in enumerate(terms):
                        stats = jnp.where(
                            lane == g * STATS + n, term[top : top + block_len], stats
                        )
            for p in range(pairs):
                out_ref[p, low : low + own_len, lanes:] = stats[
                    p * own_len : (p + 1) * own_len
                ].astype(BF16)

    vmem = pl.BlockSpec(memory_space=pltpu.VMEM)
    return pl.pallas_call(
        kernel,
        out_shape=jax.ShapeDtypeStruct((pairs, own_rows, lanes + head_dim), BF16),
        in_specs=[pl.BlockSpec(memory_space=pltpu.SMEM), vmem, vmem],
        out_specs=vmem,
        name="attend_part",
    )(where, swapped, spread)


def experts_forward(incoming, pieces):
    slots, width = incoming.shape
    counts = [piece.shape[0] for piece in pieces]
    offsets = [sum(counts[:n]) for n in range(len(pieces))]
    hidden_units = sum(counts)
    step_units = 256 if hidden_units % 256 == 0 else hidden_units

    def kernel(rows_ref, *refs):
        piece_refs = refs[: len(pieces)]
        out_ref, sum_ref, gate_ref, up_ref, down_ref, sems = refs[len(pieces) :]
        copies = [
            [
                pltpu.make_async_copy(
                    ref.at[:, pl.ds(n * width, width)],
                    target.at[pl.ds(offset, count), :],
                    sems.at[i * 3 + n],
                )
                for n, target in enumerate((gate_ref, up_ref, down_ref))
            ]
            for i, (ref, offset, count) in enumerate(zip(piece_refs, offsets, counts))
        ]
        for group in copies:
            for copy in group:
                copy.start()
        arrived = 0
        for low in range(0, hidden_units, step_units):
            while arrived < len(pieces) and offsets[arrived] < low + step_units:
                for copy in copies[arrived]:
                    copy.wait()
                arrived += 1
            span = slice(low, low + step_units)
            gate_part = dot(rows_ref[...], gate_ref[span, :], 1, 1)
            up_part = dot(rows_ref[...], up_ref[span, :], 1, 1)
            hidden = (gate_part / (1.0 + jnp.exp(-gate_part)) * up_part).astype(BF16)
            part = dot(hidden, down_ref[span, :], 1, 0)
            if low > 0:
                part = sum_ref[...] + part
            if low + step_units < hidden_units:
                sum_ref[...] = part
            else:
                out_ref[...] = part.astype(BF16)

    vmem = pl.BlockSpec(memory_space=pltpu.VMEM)
    return pl.pallas_call(
        kernel,
        out_shape=jax.ShapeDtypeStruct((slots, width), BF16),
        in_specs=[vmem] + [pl.BlockSpec(memory_space=pl.ANY)] * len(pieces),
        out_specs=vmem,
        scratch_shapes=[pltpu.VMEM((slots, width), F32)]
        + [pltpu.VMEM((hidden_units, width), BF16)] * 3
        + [pltpu.SemaphoreType.DMA((3 * len(pieces),))],
        name="experts_forward",
    )(incoming, *pieces)


def body(
    tokens_in,
    attn_gain,
    query_matrix,
    key_matrix,
    value_matrix,
    output_matrix,
    moe_gain,
    chosen_experts,
    combine_weights,
    gate_weight,
    up_weight,
    down_weight,
):
    pairs = lax.axis_size("pair")
    heads = lax.axis_size("head")
    blocks = lax.axis_size("ctx")
    seqs, own_len, width = tokens_in.shape
    own_rows = seqs * own_len
    rows = pairs * own_rows
    block_len = own_len * pairs
    q_cols = query_matrix.shape[1]
    part_cols = key_matrix.shape[0]
    head_dim = part_cols * pairs
    local_heads = q_cols // head_dim
    group = local_heads * pairs

    up_ring = [(i, (i + 1) % pairs) for i in range(pairs)]
    down_ring = [(i, (i - 1) % pairs) for i in range(pairs)]
    joined = jnp.concatenate([gate_weight[0], up_weight[0], down_weight[0]], axis=1)
    from_below = lax.ppermute(joined, "pair", up_ring)
    from_above = lax.ppermute(joined, "pair", down_ring)

    normed = normalize(tokens_in, attn_gain)
    token_send = for_each(normed, pairs)
    block_rows = exchange(token_send, "pair").reshape(rows, width)
    block_start = lax.axis_index("ctx") * block_len
    own_start = block_start + lax.axis_index("pair") * own_len
    places = jnp.arange(own_len)
    row_pos = block_start + (
        jnp.arange(pairs)[:, None, None] * own_len + jnp.zeros((seqs, 1), jnp.int32) + places
    ).reshape(rows)
    q_tables = rope_tables(row_pos.astype(F32), head_dim)
    key_value = dot(
        block_rows, jnp.concatenate([key_matrix, value_matrix], axis=0), 1, 1
    ).astype(BF16)
    query_raw = dot(block_rows, query_matrix, 1, 0)
    query = jnp.concatenate(
        [
            rotate(query_raw[:, j * head_dim : (j + 1) * head_dim], q_tables)
            for j in range(local_heads)
        ],
        axis=1,
    )
    swap_send = jnp.concatenate(
        [
            for_each(query, pairs),
            jnp.pad(
                key_value.reshape(pairs, own_rows, 2 * part_cols),
                ((0, 0), (0, 0), (0, q_cols - 2 * part_cols)),
            ),
        ],
        axis=1,
    )
    swapped = exchange(swap_send, "pair")
    own_pos = (own_start + jnp.zeros((seqs, 1), jnp.int32) + places).reshape(own_rows)
    key_own = jnp.concatenate([swapped[p, rows:, :part_cols] for p in range(pairs)], axis=1)
    value_own = jnp.concatenate(
        [swapped[p, rows:, part_cols : 2 * part_cols] for p in range(pairs)], axis=1
    )
    key_own = rotate(key_own.astype(F32), rope_tables(own_pos.astype(F32), head_dim))
    both = jnp.concatenate([key_own, value_own], axis=1)
    kv_send = for_each(both, blocks)
    spread = exchange(kv_send, "ctx")

    head = lax.axis_index("head")
    group_cols = group * head_dim
    out_mine = lax.dynamic_slice_in_dim(output_matrix, head * group_cols, group_cols, 0)
    out_theirs = lax.dynamic_slice_in_dim(
        output_matrix, (heads - 1 - head) * group_cols, group_cols, 0
    )
    out_other = lax.ppermute(
        out_theirs, "head", [(h, heads - 1 - h) for h in range(heads)]
    )

    parts = attend_part(
        jnp.stack([block_start, lax.axis_index("pair")]).astype(jnp.int32),
        swapped,
        spread,
        seqs,
        own_len,
        local_heads,
        head_dim,
    )
    merged = exchange(parts, "pair")
    part_stats = (
        merged[..., group * head_dim : group * head_dim + group * 6]
        .astype(F32)
        .reshape(pairs, own_rows, group, 6)
    )
    part_peak = jnp.sum(part_stats[..., :3], axis=-1)
    part_total = jnp.sum(part_stats[..., 3:], axis=-1)
    scale = jnp.exp(part_peak - jnp.max(part_peak, axis=0))
    scale = scale / jnp.sum(scale * part_total, axis=0)
    part_mixed = merged[..., : group * head_dim].reshape(pairs, own_rows, group, head_dim)
    attended = jnp.sum(scale[..., None] * part_mixed.astype(F32), axis=0).astype(BF16)
    attended = attended.reshape(own_rows, group * head_dim)

    gathered_heads = exchange(for_each(attended, pairs), "pair").reshape(rows, group_cols)
    projected = jnp.stack(
        [dot(gathered_heads, out_mine, 1, 0), dot(gathered_heads, out_other, 1, 0)]
    ).astype(BF16)
    out_cols = output_matrix.shape[1]
    projected = (
        projected.reshape(2, pairs, seqs, own_len, out_cols)
        .transpose(2, 1, 0, 3, 4)
        .reshape(seqs * pairs, 2 * own_len, out_cols)
    )
    owned = exchange(projected, ("head", "pair")).reshape(
        heads, pairs, 2, own_len, out_cols
    ).astype(F32)
    owned = (owned[:, :, 0] + owned[::-1, :, 1]).reshape(heads * pairs, own_len, out_cols)
    owned = jnp.moveaxis(owned, 0, 1).reshape(own_len, width)
    own_tokens = lax.dynamic_index_in_dim(tokens_in, lax.axis_index("head"), 0, keepdims=False)
    residual = (own_tokens.astype(F32) + rounded(owned)).astype(BF16)
    moe_in = normalize(residual, moe_gain)

    experts = blocks * heads
    top = chosen_experts.shape[-1]
    capacity = max(2, (own_len * top + experts - 1) // experts + 1)
    slots = experts * capacity
    picked = chosen_experts.reshape(own_len * top)
    earlier = jnp.tril(jnp.ones((own_len * top, own_len * top), jnp.bool_), -1)
    same = (picked[:, None] == picked[None, :]) & earlier
    slot_ids = picked * capacity + jnp.sum(same.astype(jnp.int32), axis=1)
    slot_ids = slot_ids.reshape(own_len, top)
    chosen_slot = slot_ids[..., None] == jnp.arange(slots)[None, None, :]
    placing = jnp.any(chosen_slot, axis=1).astype(BF16)
    outgoing = dot(placing, moe_in, 0, 0).astype(BF16)
    outgoing = outgoing.reshape(experts, capacity, width)
    incoming = exchange(outgoing, ("ctx", "head"))
    incoming = incoming.reshape(slots, width)

    half = joined.shape[0] // 2
    far_low = lax.ppermute(from_below[:half], "pair", up_ring)
    far_high = lax.ppermute(from_above[half:], "pair", down_ring)
    expert_out = experts_forward(incoming, [joined, from_below, from_above, far_low, far_high])
    returned = exchange(expert_out.reshape(experts, capacity, width), ("ctx", "head"))
    returned = returned.reshape(slots, width)
    share = jnp.sum(
        jnp.where(chosen_slot, combine_weights.reshape(own_len, top, 1), 0.0), axis=1
    )
    high = rounded(share)
    mixture = dot(jnp.concatenate([high, share - high], axis=0).astype(BF16), returned, 1, 0)
    mixture = mixture[:own_len] + mixture[own_len:]
    return (residual.astype(F32) + mixture).astype(BF16)[None]


def solution(mesh):
    return jax.shard_map(
        body,
        mesh=mesh,
        in_specs=(
            P(None, ("ctx", "pair"), None),
            P(),
            P(None, ("head", "pair")),
            P(("head", "pair"), None),
            P(("head", "pair"), None),
            P(None, ("head", "pair")),
            P(),
            P("head", ("ctx", "pair"), None),
            P("head", ("ctx", "pair"), None),
            P(("ctx", "head"), "pair", None),
            P(("ctx", "head"), "pair", None),
            P(("ctx", "head"), "pair", None),
        ),
        out_specs=P("head", ("ctx", "pair"), None),
        check_vma=False,
    )
```

```python
import jax
import jax.numpy as jnp
from jax import lax
from jax.experimental import pallas as pl
from jax.experimental.pallas import tpu as pltpu
from jax.sharding import PartitionSpec as P


ROPE_BASE = 1000000.0
EPSILON = 1e-06
MASKED = -1e30
F32 = jnp.float32
BF16 = jnp.bfloat16


def exchange(tiles, axis):
    return lax.all_to_all(tiles, axis, 0, 0, tiled=True)


def for_each(shard, count):
    return jnp.broadcast_to(shard[None], (count, *shard.shape))


def dot(a, b, a_dim, b_dim):
    return lax.dot_general(a, b, (((a_dim,), (b_dim,)), ((), ())), preferred_element_type=F32)


def normalize(values, gain_vector):
    wide = values.astype(F32)
    mean_square = jnp.mean(wide * wide, axis=-1, keepdims=True)
    return (wide * lax.rsqrt(mean_square + EPSILON) * gain_vector).astype(BF16)


def rope_tables(positions, head_dim):
    half_dim = head_dim // 2
    frequency = ROPE_BASE ** (-(jnp.arange(half_dim).astype(F32) * 2.0) / head_dim)
    angles = positions[:, None] * frequency[None, :]
    return jnp.cos(angles), jnp.sin(angles)


def rotate(values, tables):
    cosine_part, sine_part = tables
    half_dim = values.shape[-1] // 2
    lower_half = values[..., :half_dim]
    upper_half = values[..., half_dim:]
    return jnp.concatenate(
        [
            lower_half * cosine_part - upper_half * sine_part,
            upper_half * cosine_part + lower_half * sine_part,
        ],
        axis=-1,
    ).astype(BF16)


def rounded(values):
    return lax.reduce_precision(values, 8, 7)


STATS = 6
LOG2_E = 1.4426950408889634
GROUP_ROWS = 256
WHOLE_VMEM = 66_500_000


def attend_part(where, swapped, spread, seqs, own_len, local_heads, head_dim):
    pairs = swapped.shape[0]
    own_rows = seqs * own_len
    block_len = pairs * own_len
    blocks = spread.shape[0]
    group = pairs * local_heads
    lanes = group * head_dim
    scaling = head_dim ** (-0.5)
    heads_each = GROUP_ROWS // block_len

    def kernel(where_ref, swapped_ref, spread_ref, out_ref):
        start = where_ref[0]
        me = where_ref[1]
        key_index = lax.broadcasted_iota(jnp.int32, (1, blocks * own_len), 1)
        key_pos = (key_index // own_len) * block_len + me * own_len + key_index % own_len
        row = lax.broadcasted_iota(jnp.int32, (GROUP_ROWS, 1), 0)
        allowed = key_pos <= start + row % block_len
        lane = lax.broadcasted_iota(jnp.int32, (block_len, head_dim), 1)
        for seq in range(seqs):
            low = seq * own_len
            keys = spread_ref[:, low : low + own_len, :head_dim].reshape(-1, head_dim)
            values = spread_ref[:, low : low + own_len, head_dim:].reshape(-1, head_dim)
            stats = jnp.zeros((block_len, head_dim), F32)
            for first in range(0, group, heads_each):
                query = jnp.concatenate(
                    [
                        swapped_ref[
                            g // local_heads,
                            p * own_rows + low : p * own_rows + low + own_len,
                            (g % local_heads) * head_dim : (g % local_heads + 1) * head_dim,
                        ]
                        for g in range(first, first + heads_each)
                        for p in range(pairs)
                    ],
                    axis=0,
                )
                scores = jnp.where(allowed, dot(query, keys, 1, 1), MASKED)
                peak = jnp.maximum(jnp.max(scores, axis=1, keepdims=True), 0.1 * MASKED)
                probs = jnp.exp2((scores - peak) * (scaling * LOG2_E))
                total = jnp.sum(probs, axis=1, keepdims=True)
                mixed = dot(probs.astype(BF16), values, 1, 0).astype(BF16)
                terms = []
                for number in (peak * scaling, total):
                    high = number.astype(BF16).astype(F32)
                    middle = (number - high).astype(BF16).astype(F32)
                    terms += [high, middle, number - high - middle]
                for g in range(first, first + heads_each):
                    top = (g - first) * block_len
                    for p in range(pairs):
                        at = top + p * own_len
                        out_ref[
                            p, low : low + own_len, g * head_dim : (g + 1) * head_dim
                        ] = mixed[at : at + own_len]
                    for n, term in enumerate(terms):
                        stats = jnp.where(
                            lane == g * STATS + n, term[top : top + block_len], stats
                        )
            for p in range(pairs):
                out_ref[p, low : low + own_len, lanes:] = stats[
                    p * own_len : (p + 1) * own_len
                ].astype(BF16)

    vmem = pl.BlockSpec(memory_space=pltpu.VMEM)
    return pl.pallas_call(
        kernel,
        out_shape=jax.ShapeDtypeStruct((pairs, own_rows, lanes + head_dim), BF16),
        in_specs=[pl.BlockSpec(memory_space=pltpu.SMEM), vmem, vmem],
        out_specs=vmem,
        compiler_params=pltpu.CompilerParams(vmem_limit_bytes=WHOLE_VMEM),
        name="attend_part",
    )(where, swapped, spread)


def experts_forward(incoming, pieces):
    slots, width = incoming.shape
    counts = [piece.shape[0] for piece in pieces]
    offsets = [sum(counts[:n]) for n in range(len(pieces))]
    hidden_units = sum(counts)
    step_units = 256 if hidden_units % 256 == 0 else hidden_units

    def kernel(rows_ref, *refs):
        piece_refs = refs[: len(pieces)]
        out_ref, sum_ref, gate_ref, up_ref, down_ref, sems = refs[len(pieces) :]
        copies = [
            [
                pltpu.make_async_copy(
                    ref.at[:, pl.ds(n * width, width)],
                    target.at[pl.ds(offset, count), :],
                    sems.at[i * 3 + n],
                )
                for n, target in enumerate((gate_ref, up_ref, down_ref))
            ]
            for i, (ref, offset, count) in enumerate(zip(piece_refs, offsets, counts))
        ]
        for group in copies:
            for copy in group:
                copy.start()
        arrived = 0
        for low in range(0, hidden_units, step_units):
            while arrived < len(pieces) and offsets[arrived] < low + step_units:
                for copy in copies[arrived]:
                    copy.wait()
                arrived += 1
            span = slice(low, low + step_units)
            gate_part = dot(rows_ref[...], gate_ref[span, :], 1, 1)
            up_part = dot(rows_ref[...], up_ref[span, :], 1, 1)
            hidden = (gate_part / (1.0 + jnp.exp(-gate_part)) * up_part).astype(BF16)
            part = dot(hidden, down_ref[span, :], 1, 0)
            if low > 0:
                part = sum_ref[...] + part
            if low + step_units < hidden_units:
                sum_ref[...] = part
            else:
                out_ref[...] = part.astype(BF16)

    vmem = pl.BlockSpec(memory_space=pltpu.VMEM)
    return pl.pallas_call(
        kernel,
        out_shape=jax.ShapeDtypeStruct((slots, width), BF16),
        in_specs=[vmem] + [pl.BlockSpec(memory_space=pltpu.HBM)] * len(pieces),
        out_specs=vmem,
        scratch_shapes=[pltpu.VMEM((slots, width), F32)]
        + [pltpu.VMEM((hidden_units, width), BF16)] * 3
        + [pltpu.SemaphoreType.DMA((3 * len(pieces),))],
        name="experts_forward",
    )(incoming, *pieces)


def side_by_side(arrays, after):
    count, width = arrays[0].shape

    def kernel(*refs):
        out_ref, sems = refs[len(arrays) + 1 :]
        copies = [
            pltpu.make_async_copy(ref, out_ref.at[:, pl.ds(n * width, width)], sems.at[n])
            for n, ref in enumerate(refs[: len(arrays)])
        ]
        for copy in copies:
            copy.start()
        for copy in copies:
            copy.wait()

    hbm = pl.BlockSpec(memory_space=pltpu.HBM)
    return pl.pallas_call(
        kernel,
        out_shape=jax.ShapeDtypeStruct((count, width * len(arrays)), arrays[0].dtype),
        in_specs=[hbm] * (len(arrays) + 1),
        out_specs=hbm,
        scratch_shapes=[pltpu.SemaphoreType.DMA((len(arrays),))],
        name="side_by_side",
    )(*arrays, after)


def halves(low_source, high_source):
    count, width = low_source.shape
    half = count // 2

    def kernel(low_ref, high_ref, low_out, high_out, sems):
        copies = [
            pltpu.make_async_copy(low_ref.at[pl.ds(0, half), :], low_out, sems.at[0]),
            pltpu.make_async_copy(
                high_ref.at[pl.ds(half, count - half), :], high_out, sems.at[1]
            ),
        ]
        for copy in copies:
            copy.start()
        for copy in copies:
            copy.wait()

    hbm = pl.BlockSpec(memory_space=pltpu.HBM)
    return pl.pallas_call(
        kernel,
        out_shape=(
            jax.ShapeDtypeStruct((half, width), low_source.dtype),
            jax.ShapeDtypeStruct((count - half, width), high_source.dtype),
        ),
        in_specs=[hbm, hbm],
        out_specs=(hbm, hbm),
        scratch_shapes=[pltpu.SemaphoreType.DMA((2,))],
        name="halves",
    )(low_source, high_source)


def body(
    tokens_in,
    attn_gain,
    query_matrix,
    key_matrix,
    value_matrix,
    output_matrix,
    moe_gain,
    chosen_experts,
    combine_weights,
    gate_weight,
    up_weight,
    down_weight,
):
    pairs = lax.axis_size("pair")
    heads = lax.axis_size("head")
    blocks = lax.axis_size("ctx")
    seqs, own_len, width = tokens_in.shape
    own_rows = seqs * own_len
    rows = pairs * own_rows
    block_len = own_len * pairs
    q_cols = query_matrix.shape[1]
    part_cols = key_matrix.shape[0]
    head_dim = part_cols * pairs
    local_heads = q_cols // head_dim
    group = local_heads * pairs

    normed = normalize(tokens_in, attn_gain)
    token_send = for_each(normed, pairs)
    block_rows = exchange(token_send, "pair").reshape(rows, width)
    block_start = lax.axis_index("ctx") * block_len
    own_start = block_start + lax.axis_index("pair") * own_len
    places = jnp.arange(own_len)
    row_pos = block_start + (
        jnp.arange(pairs)[:, None, None] * own_len + jnp.zeros((seqs, 1), jnp.int32) + places
    ).reshape(rows)
    q_tables = rope_tables(row_pos.astype(F32), head_dim)
    key_value = dot(
        block_rows, jnp.concatenate([key_matrix, value_matrix], axis=0), 1, 1
    ).astype(BF16)
    query_raw = dot(block_rows, query_matrix, 1, 0)
    query = jnp.concatenate(
        [
            rotate(query_raw[:, j * head_dim : (j + 1) * head_dim], q_tables)
            for j in range(local_heads)
        ],
        axis=1,
    )
    swap_send = jnp.concatenate(
        [
            for_each(query, pairs),
            jnp.pad(
                key_value.reshape(pairs, own_rows, 2 * part_cols),
                ((0, 0), (0, 0), (0, q_cols - 2 * part_cols)),
            ),
        ],
        axis=1,
    )
    up_ring = [(i, (i + 1) % pairs) for i in range(pairs)]
    down_ring = [(i, (i - 1) % pairs) for i in range(pairs)]
    joined = side_by_side([gate_weight[0], up_weight[0], down_weight[0]], swap_send)
    from_below = lax.ppermute(joined, "pair", up_ring)
    from_above = lax.ppermute(joined, "pair", down_ring)

    swapped = exchange(swap_send, "pair")
    own_pos = (own_start + jnp.zeros((seqs, 1), jnp.int32) + places).reshape(own_rows)
    key_own = jnp.concatenate([swapped[p, rows:, :part_cols] for p in range(pairs)], axis=1)
    value_own = jnp.concatenate(
        [swapped[p, rows:, part_cols : 2 * part_cols] for p in range(pairs)], axis=1
    )
    key_own = rotate(key_own.astype(F32), rope_tables(own_pos.astype(F32), head_dim))
    both = jnp.concatenate([key_own, value_own], axis=1)
    kv_send = for_each(both, blocks)
    spread = exchange(kv_send, "ctx")

    head = lax.axis_index("head")
    group_cols = group * head_dim
    out_mine = lax.dynamic_slice_in_dim(output_matrix, head * group_cols, group_cols, 0)
    out_theirs = lax.dynamic_slice_in_dim(
        output_matrix, (heads - 1 - head) * group_cols, group_cols, 0
    )
    out_other = lax.ppermute(
        out_theirs, "head", [(h, heads - 1 - h) for h in range(heads)]
    )

    parts = attend_part(
        jnp.stack([block_start, lax.axis_index("pair")]).astype(jnp.int32),
        swapped,
        spread,
        seqs,
        own_len,
        local_heads,
        head_dim,
    )
    merged = exchange(parts, "pair")
    part_stats = (
        merged[..., group * head_dim : group * head_dim + group * 6]
        .astype(F32)
        .reshape(pairs, own_rows, group, 6)
    )
    part_peak = jnp.sum(part_stats[..., :3], axis=-1)
    part_total = jnp.sum(part_stats[..., 3:], axis=-1)
    scale = jnp.exp(part_peak - jnp.max(part_peak, axis=0))
    scale = scale / jnp.sum(scale * part_total, axis=0)
    part_mixed = merged[..., : group * head_dim].reshape(pairs, own_rows, group, head_dim)
    attended = jnp.sum(scale[..., None] * part_mixed.astype(F32), axis=0).astype(BF16)
    attended = attended.reshape(own_rows, group * head_dim)

    heads_send = for_each(attended, pairs)
    gathered_heads = exchange(heads_send, "pair").reshape(rows, group_cols)
    projected = jnp.stack(
        [dot(gathered_heads, out_mine, 1, 0), dot(gathered_heads, out_other, 1, 0)]
    ).astype(BF16)
    out_cols = output_matrix.shape[1]
    projected = (
        projected.reshape(2, pairs, seqs, own_len, out_cols)
        .transpose(2, 1, 0, 3, 4)
        .reshape(seqs * pairs, 2 * own_len, out_cols)
    )
    owned = exchange(projected, ("head", "pair"))
    owned = owned.reshape(heads, pairs, 2, own_len, out_cols).astype(F32)
    owned = (owned[:, :, 0] + owned[::-1, :, 1]).reshape(heads * pairs, own_len, out_cols)
    owned = jnp.moveaxis(owned, 0, 1).reshape(own_len, width)
    own_tokens = lax.dynamic_index_in_dim(tokens_in, lax.axis_index("head"), 0, keepdims=False)
    residual = (own_tokens.astype(F32) + rounded(owned)).astype(BF16)
    moe_in = normalize(residual, moe_gain)

    experts = blocks * heads
    top = chosen_experts.shape[-1]
    capacity = max(2, (own_len * top + experts - 1) // experts + 1)
    slots = experts * capacity
    picked = chosen_experts.reshape(own_len * top)
    earlier = jnp.tril(jnp.ones((own_len * top, own_len * top), jnp.bool_), -1)
    same = (picked[:, None] == picked[None, :]) & earlier
    slot_ids = picked * capacity + jnp.sum(same.astype(jnp.int32), axis=1)
    slot_ids = slot_ids.reshape(own_len, top)
    chosen_slot = slot_ids[..., None] == jnp.arange(slots)[None, None, :]
    placing = jnp.any(chosen_slot, axis=1).astype(BF16)
    outgoing = dot(placing, moe_in, 0, 0).astype(BF16)
    outgoing = outgoing.reshape(experts, capacity, width)
    incoming = exchange(outgoing, ("ctx", "head"))
    incoming = incoming.reshape(slots, width)

    low_half, high_half = halves(from_below, from_above)
    far_low = lax.ppermute(low_half, "pair", up_ring)
    far_high = lax.ppermute(high_half, "pair", down_ring)
    expert_out = experts_forward(incoming, [joined, from_below, from_above, far_low, far_high])
    returned = exchange(expert_out.reshape(experts, capacity, width), ("ctx", "head"))
    returned = returned.reshape(slots, width)
    share = jnp.sum(
        jnp.where(chosen_slot, combine_weights.reshape(own_len, top, 1), 0.0), axis=1
    )
    high = rounded(share)
    mixture = dot(jnp.concatenate([high, share - high], axis=0).astype(BF16), returned, 1, 0)
    mixture = mixture[:own_len] + mixture[own_len:]
    return (residual.astype(F32) + mixture).astype(BF16)[None]


def solution(mesh):
    return jax.shard_map(
        body,
        mesh=mesh,
        in_specs=(
            P(None, ("ctx", "pair"), None),
            P(),
            P(None, ("head", "pair")),
            P(("head", "pair"), None),
            P(("head", "pair"), None),
            P(None, ("head", "pair")),
            P(),
            P("head", ("ctx", "pair"), None),
            P("head", ("ctx", "pair"), None),
            P(("ctx", "head"), "pair", None),
            P(("ctx", "head"), "pair", None),
            P(("ctx", "head"), "pair", None),
        ),
        out_specs=P("head", ("ctx", "pair"), None),
        check_vma=False,
    )
```

```python
import jax
import jax.numpy as jnp
from jax import lax
from jax.experimental import pallas as pl
from jax.experimental.pallas import tpu as pltpu
from jax.sharding import PartitionSpec as P


ROPE_BASE = 1000000.0
EPSILON = 1e-06
MASKED = -1e30
F32 = jnp.float32
BF16 = jnp.bfloat16


def exchange(tiles, axis):
    return lax.all_to_all(tiles, axis, 0, 0, tiled=True)


def for_each(shard, count):
    return jnp.broadcast_to(shard[None], (count, *shard.shape))


def dot(a, b, a_dim, b_dim):
    return lax.dot_general(a, b, (((a_dim,), (b_dim,)), ((), ())), preferred_element_type=F32)


def normalize(values, gain_vector):
    wide = values.astype(F32)
    mean_square = jnp.mean(wide * wide, axis=-1, keepdims=True)
    return (wide * lax.rsqrt(mean_square + EPSILON) * gain_vector).astype(BF16)


def rope_tables(positions, head_dim):
    half_dim = head_dim // 2
    frequency = ROPE_BASE ** (-(jnp.arange(half_dim).astype(F32) * 2.0) / head_dim)
    angles = positions[:, None] * frequency[None, :]
    return jnp.cos(angles), jnp.sin(angles)


def rotate(values, tables):
    cosine_part, sine_part = tables
    half_dim = values.shape[-1] // 2
    lower_half = values[..., :half_dim]
    upper_half = values[..., half_dim:]
    return jnp.concatenate(
        [
            lower_half * cosine_part - upper_half * sine_part,
            upper_half * cosine_part + lower_half * sine_part,
        ],
        axis=-1,
    ).astype(BF16)


def rounded(values):
    return lax.reduce_precision(values, 8, 7)


STATS = 6
LOG2_E = 1.4426950408889634
GROUP_ROWS = 256
WHOLE_VMEM = 66_500_000


def attend_part(where, swapped, spread, seqs, own_len, local_heads, head_dim):
    pairs = swapped.shape[0]
    own_rows = seqs * own_len
    block_len = pairs * own_len
    blocks = spread.shape[0]
    group = pairs * local_heads
    lanes = group * head_dim
    scaling = head_dim ** (-0.5)
    heads_each = GROUP_ROWS // block_len

    def kernel(where_ref, swapped_ref, spread_ref, out_ref):
        start = where_ref[0]
        me = where_ref[1]
        key_index = lax.broadcasted_iota(jnp.int32, (1, blocks * own_len), 1)
        key_pos = (key_index // own_len) * block_len + me * own_len + key_index % own_len
        row = lax.broadcasted_iota(jnp.int32, (GROUP_ROWS, 1), 0)
        allowed = key_pos <= start + row % block_len
        lane = lax.broadcasted_iota(jnp.int32, (block_len, head_dim), 1)
        for seq in range(seqs):
            low = seq * own_len
            keys = spread_ref[:, low : low + own_len, :head_dim].reshape(-1, head_dim)
            values = spread_ref[:, low : low + own_len, head_dim:].reshape(-1, head_dim)
            stats = jnp.zeros((block_len, head_dim), F32)
            for first in range(0, group, heads_each):
                query = jnp.concatenate(
                    [
                        swapped_ref[
                            g // local_heads,
                            p * own_rows + low : p * own_rows + low + own_len,
                            (g % local_heads) * head_dim : (g % local_heads + 1) * head_dim,
                        ]
                        for g in range(first, first + heads_each)
                        for p in range(pairs)
                    ],
                    axis=0,
                )
                scores = jnp.where(allowed, dot(query, keys, 1, 1), MASKED)
                peak = jnp.maximum(jnp.max(scores, axis=1, keepdims=True), 0.1 * MASKED)
                probs = jnp.exp2((scores - peak) * (scaling * LOG2_E))
                total = jnp.sum(probs, axis=1, keepdims=True)
                mixed = dot(probs.astype(BF16), values, 1, 0).astype(BF16)
                terms = []
                for number in (peak * scaling, total):
                    high = number.astype(BF16).astype(F32)
                    middle = (number - high).astype(BF16).astype(F32)
                    terms += [high, middle, number - high - middle]
                for g in range(first, first + heads_each):
                    top = (g - first) * block_len
                    for p in range(pairs):
                        at = top + p * own_len
                        out_ref[
                            p, low : low + own_len, g * head_dim : (g + 1) * head_dim
                        ] = mixed[at : at + own_len]
                    for n, term in enumerate(terms):
                        stats = jnp.where(
                            lane == g * STATS + n, term[top : top + block_len], stats
                        )
            for p in range(pairs):
                out_ref[p, low : low + own_len, lanes:] = stats[
                    p * own_len : (p + 1) * own_len
                ].astype(BF16)

    vmem = pl.BlockSpec(memory_space=pltpu.VMEM)
    return pl.pallas_call(
        kernel,
        out_shape=jax.ShapeDtypeStruct((pairs, own_rows, lanes + head_dim), BF16),
        in_specs=[pl.BlockSpec(memory_space=pltpu.SMEM), vmem, vmem],
        out_specs=vmem,
        compiler_params=pltpu.CompilerParams(vmem_limit_bytes=WHOLE_VMEM),
        name="attend_part",
    )(where, swapped, spread)


def experts_forward(incoming, pieces):
    slots, width = incoming.shape
    counts = [piece.shape[0] for piece in pieces]
    offsets = [sum(counts[:n]) for n in range(len(pieces))]
    hidden_units = sum(counts)
    step_units = 256 if hidden_units % 256 == 0 else hidden_units

    def kernel(rows_ref, *refs):
        piece_refs = refs[: len(pieces)]
        out_ref, sum_ref, gate_ref, up_ref, down_ref, sems = refs[len(pieces) :]
        copies = [
            [
                pltpu.make_async_copy(
                    ref.at[:, pl.ds(n * width, width)],
                    target.at[pl.ds(offset, count), :],
                    sems.at[i * 3 + n],
                )
                for n, target in enumerate((gate_ref, up_ref, down_ref))
            ]
            for i, (ref, offset, count) in enumerate(zip(piece_refs, offsets, counts))
        ]
        for group in copies:
            for copy in group:
                copy.start()
        arrived = 0
        for low in range(0, hidden_units, step_units):
            while arrived < len(pieces) and offsets[arrived] < low + step_units:
                for copy in copies[arrived]:
                    copy.wait()
                arrived += 1
            span = slice(low, low + step_units)
            gate_part = dot(rows_ref[...], gate_ref[span, :], 1, 1)
            up_part = dot(rows_ref[...], up_ref[span, :], 1, 1)
            hidden = (gate_part / (1.0 + jnp.exp(-gate_part)) * up_part).astype(BF16)
            part = dot(hidden, down_ref[span, :], 1, 0)
            if low > 0:
                part = sum_ref[...] + part
            if low + step_units < hidden_units:
                sum_ref[...] = part
            else:
                out_ref[...] = part.astype(BF16)

    vmem = pl.BlockSpec(memory_space=pltpu.VMEM)
    return pl.pallas_call(
        kernel,
        out_shape=jax.ShapeDtypeStruct((slots, width), BF16),
        in_specs=[vmem] + [pl.BlockSpec(memory_space=pltpu.HBM)] * len(pieces),
        out_specs=vmem,
        scratch_shapes=[pltpu.VMEM((slots, width), F32)]
        + [pltpu.VMEM((hidden_units, width), BF16)] * 3
        + [pltpu.SemaphoreType.DMA((3 * len(pieces),))],
        name="experts_forward",
    )(incoming, *pieces)


def body(
    tokens_in,
    attn_gain,
    query_matrix,
    key_matrix,
    value_matrix,
    output_matrix,
    moe_gain,
    chosen_experts,
    combine_weights,
    gate_weight,
    up_weight,
    down_weight,
):
    pairs = lax.axis_size("pair")
    heads = lax.axis_size("head")
    blocks = lax.axis_size("ctx")
    seqs, own_len, width = tokens_in.shape
    own_rows = seqs * own_len
    rows = pairs * own_rows
    block_len = own_len * pairs
    q_cols = query_matrix.shape[1]
    part_cols = key_matrix.shape[0]
    head_dim = part_cols * pairs
    local_heads = q_cols // head_dim
    group = local_heads * pairs

    up_ring = [(i, (i + 1) % pairs) for i in range(pairs)]
    down_ring = [(i, (i - 1) % pairs) for i in range(pairs)]
    joined = jnp.concatenate([gate_weight[0], up_weight[0], down_weight[0]], axis=1)
    from_below = lax.ppermute(joined, "pair", up_ring)
    from_above = lax.ppermute(joined, "pair", down_ring)

    normed = normalize(tokens_in, attn_gain)
    token_send = for_each(normed, pairs)
    block_rows = exchange(token_send, "pair").reshape(rows, width)
    block_start = lax.axis_index("ctx") * block_len
    own_start = block_start + lax.axis_index("pair") * own_len
    places = jnp.arange(own_len)
    row_pos = block_start + (
        jnp.arange(pairs)[:, None, None] * own_len + jnp.zeros((seqs, 1), jnp.int32) + places
    ).reshape(rows)
    q_tables = rope_tables(row_pos.astype(F32), head_dim)
    key_value = dot(
        block_rows, jnp.concatenate([key_matrix, value_matrix], axis=0), 1, 1
    ).astype(BF16)
    query_raw = dot(block_rows, query_matrix, 1, 0)
    query = jnp.concatenate(
        [
            rotate(query_raw[:, j * head_dim : (j + 1) * head_dim], q_tables)
            for j in range(local_heads)
        ],
        axis=1,
    )
    swap_send = jnp.concatenate(
        [
            for_each(query, pairs),
            jnp.pad(
                key_value.reshape(pairs, own_rows, 2 * part_cols),
                ((0, 0), (0, 0), (0, q_cols - 2 * part_cols)),
            ),
        ],
        axis=1,
    )
    swapped = exchange(swap_send, "pair")
    own_pos = (own_start + jnp.zeros((seqs, 1), jnp.int32) + places).reshape(own_rows)
    key_own = jnp.concatenate([swapped[p, rows:, :part_cols] for p in range(pairs)], axis=1)
    value_own = jnp.concatenate(
        [swapped[p, rows:, part_cols : 2 * part_cols] for p in range(pairs)], axis=1
    )
    key_own = rotate(key_own.astype(F32), rope_tables(own_pos.astype(F32), head_dim))
    both = jnp.concatenate([key_own, value_own], axis=1)
    kv_send = for_each(both, blocks)
    spread = exchange(kv_send, "ctx")

    head = lax.axis_index("head")
    group_cols = group * head_dim
    out_mine = lax.dynamic_slice_in_dim(output_matrix, head * group_cols, group_cols, 0)
    out_theirs = lax.dynamic_slice_in_dim(
        output_matrix, (heads - 1 - head) * group_cols, group_cols, 0
    )
    out_other = lax.ppermute(
        out_theirs, "head", [(h, heads - 1 - h) for h in range(heads)]
    )

    parts = attend_part(
        jnp.stack([block_start, lax.axis_index("pair")]).astype(jnp.int32),
        swapped,
        spread,
        seqs,
        own_len,
        local_heads,
        head_dim,
    )
    merged = exchange(parts, "pair")
    part_stats = (
        merged[..., group * head_dim : group * head_dim + group * 6]
        .astype(F32)
        .reshape(pairs, own_rows, group, 6)
    )
    part_peak = jnp.sum(part_stats[..., :3], axis=-1)
    part_total = jnp.sum(part_stats[..., 3:], axis=-1)
    scale = jnp.exp(part_peak - jnp.max(part_peak, axis=0))
    scale = scale / jnp.sum(scale * part_total, axis=0)
    part_mixed = merged[..., : group * head_dim].reshape(pairs, own_rows, group, head_dim)
    attended = jnp.sum(scale[..., None] * part_mixed.astype(F32), axis=0).astype(BF16)
    attended = attended.reshape(own_rows, group * head_dim)

    heads_send = for_each(attended, pairs)
    gathered_heads = exchange(heads_send, "pair").reshape(rows, group_cols)
    projected = jnp.stack(
        [dot(gathered_heads, out_mine, 1, 0), dot(gathered_heads, out_other, 1, 0)]
    ).astype(BF16)
    out_cols = output_matrix.shape[1]
    projected = (
        projected.reshape(2, pairs, seqs, own_len, out_cols)
        .transpose(2, 1, 0, 3, 4)
        .reshape(seqs * pairs, 2 * own_len, out_cols)
    )
    owned = exchange(projected, ("head", "pair"))
    owned = owned.reshape(heads, pairs, 2, own_len, out_cols).astype(F32)
    owned = (owned[:, :, 0] + owned[::-1, :, 1]).reshape(heads * pairs, own_len, out_cols)
    owned = jnp.moveaxis(owned, 0, 1).reshape(own_len, width)
    own_tokens = lax.dynamic_index_in_dim(tokens_in, lax.axis_index("head"), 0, keepdims=False)
    residual = (own_tokens.astype(F32) + rounded(owned)).astype(BF16)
    moe_in = normalize(residual, moe_gain)

    experts = blocks * heads
    top = chosen_experts.shape[-1]
    capacity = max(2, (own_len * top + experts - 1) // experts + 1)
    slots = experts * capacity
    picked = chosen_experts.reshape(own_len * top)
    earlier = jnp.tril(jnp.ones((own_len * top, own_len * top), jnp.bool_), -1)
    same = (picked[:, None] == picked[None, :]) & earlier
    slot_ids = picked * capacity + jnp.sum(same.astype(jnp.int32), axis=1)
    slot_ids = slot_ids.reshape(own_len, top)
    chosen_slot = slot_ids[..., None] == jnp.arange(slots)[None, None, :]
    placing = jnp.any(chosen_slot, axis=1).astype(BF16)
    outgoing = dot(placing, moe_in, 0, 0).astype(BF16)
    outgoing = outgoing.reshape(experts, capacity, width)
    incoming = exchange(outgoing, ("ctx", "head"))
    incoming = incoming.reshape(slots, width)

    half = joined.shape[0] // 2
    low_half = from_below[:half]
    high_half = from_above[half:]
    far_low = lax.ppermute(low_half, "pair", up_ring)
    far_high = lax.ppermute(high_half, "pair", down_ring)
    expert_out = experts_forward(incoming, [joined, from_below, from_above, far_low, far_high])
    returned = exchange(expert_out.reshape(experts, capacity, width), ("ctx", "head"))
    returned = returned.reshape(slots, width)
    share = jnp.sum(
        jnp.where(chosen_slot, combine_weights.reshape(own_len, top, 1), 0.0), axis=1
    )
    high = rounded(share)
    mixture = dot(jnp.concatenate([high, share - high], axis=0).astype(BF16), returned, 1, 0)
    mixture = mixture[:own_len] + mixture[own_len:]
    return (residual.astype(F32) + mixture).astype(BF16)[None]


def solution(mesh):
    return jax.shard_map(
        body,
        mesh=mesh,
        in_specs=(
            P(None, ("ctx", "pair"), None),
            P(),
            P(None, ("head", "pair")),
            P(("head", "pair"), None),
            P(("head", "pair"), None),
            P(None, ("head", "pair")),
            P(),
            P("head", ("ctx", "pair"), None),
            P("head", ("ctx", "pair"), None),
            P(("ctx", "head"), "pair", None),
            P(("ctx", "head"), "pair", None),
            P(("ctx", "head"), "pair", None),
        ),
        out_specs=P("head", ("ctx", "pair"), None),
        check_vma=False,
    )
```

```python
import math

import jax
import jax.numpy as jnp
from jax import lax
from jax.experimental import pallas as pl
from jax.experimental.pallas import tpu as pltpu
from jax.sharding import PartitionSpec as P


ROPE_BASE = 1000000.0
EPSILON = 1e-06
MASKED = -1e30
F32 = jnp.float32
BF16 = jnp.bfloat16


def exchange(tiles, axis, groups=None):
    return lax.all_to_all(tiles, axis, 0, 0, tiled=True, axis_index_groups=groups)


def for_each(shard, count):
    return jnp.broadcast_to(shard[None], (count, *shard.shape))


def dot(a, b, a_dim, b_dim):
    return lax.dot_general(a, b, (((a_dim,), (b_dim,)), ((), ())), preferred_element_type=F32)


def normalize(values, gain_vector):
    wide = values.astype(F32)
    mean_square = jnp.mean(wide * wide, axis=-1, keepdims=True)
    return (wide * lax.rsqrt(mean_square + EPSILON) * gain_vector).astype(BF16)


def rope_tables(positions, head_dim):
    half_dim = head_dim // 2
    frequency = ROPE_BASE ** (-(jnp.arange(half_dim).astype(F32) * 2.0) / head_dim)
    angles = positions[:, None] * frequency[None, :]
    return jnp.cos(angles), jnp.sin(angles)


def rotate(values, tables):
    cosine_part, sine_part = tables
    half_dim = values.shape[-1] // 2
    lower_half = values[..., :half_dim]
    upper_half = values[..., half_dim:]
    return jnp.concatenate(
        [
            lower_half * cosine_part - upper_half * sine_part,
            upper_half * cosine_part + lower_half * sine_part,
        ],
        axis=-1,
    ).astype(BF16)


def rounded(values):
    return lax.reduce_precision(values, 8, 7)


STATS = 6
LOG2_E = 1.4426950408889634
GROUP_ROWS = 256
WHOLE_VMEM = 66_500_000


def attend_part(where, swapped, spread, seqs, own_len, local_heads, head_dim):
    pairs = swapped.shape[0]
    own_rows = seqs * own_len
    block_len = pairs * own_len
    blocks = spread.shape[0]
    group = pairs * local_heads
    lanes = group * head_dim
    scaling = head_dim ** (-0.5)
    heads_each = GROUP_ROWS // block_len

    def kernel(where_ref, swapped_ref, spread_ref, out_ref):
        start = where_ref[0]
        me = where_ref[1]
        key_index = lax.broadcasted_iota(jnp.int32, (1, blocks * own_len), 1)
        key_pos = (key_index // own_len) * block_len + me * own_len + key_index % own_len
        row = lax.broadcasted_iota(jnp.int32, (GROUP_ROWS, 1), 0)
        allowed = key_pos <= start + row % block_len
        lane = lax.broadcasted_iota(jnp.int32, (block_len, head_dim), 1)
        for seq in range(seqs):
            low = seq * own_len
            keys = spread_ref[:, low : low + own_len, :head_dim].reshape(-1, head_dim)
            values = spread_ref[:, low : low + own_len, head_dim:].reshape(-1, head_dim)
            stats = jnp.zeros((block_len, head_dim), F32)
            for first in range(0, group, heads_each):
                query = jnp.concatenate(
                    [
                        swapped_ref[
                            g // local_heads,
                            p * own_rows + low : p * own_rows + low + own_len,
                            (g % local_heads) * head_dim : (g % local_heads + 1) * head_dim,
                        ]
                        for g in range(first, first + heads_each)
                        for p in range(pairs)
                    ],
                    axis=0,
                )
                scores = jnp.where(allowed, dot(query, keys, 1, 1), MASKED)
                peak = jnp.maximum(jnp.max(scores, axis=1, keepdims=True), 0.1 * MASKED)
                probs = jnp.exp2((scores - peak) * (scaling * LOG2_E))
                total = jnp.sum(probs, axis=1, keepdims=True)
                mixed = dot(probs.astype(BF16), values, 1, 0).astype(BF16)
                terms = []
                for number in (peak * scaling, total):
                    high = number.astype(BF16).astype(F32)
                    middle = (number - high).astype(BF16).astype(F32)
                    terms += [high, middle, number - high - middle]
                for g in range(first, first + heads_each):
                    top = (g - first) * block_len
                    for p in range(pairs):
                        at = top + p * own_len
                        out_ref[
                            p, low : low + own_len, g * head_dim : (g + 1) * head_dim
                        ] = mixed[at : at + own_len]
                    for n, term in enumerate(terms):
                        stats = jnp.where(
                            lane == g * STATS + n, term[top : top + block_len], stats
                        )
            for p in range(pairs):
                out_ref[p, low : low + own_len, lanes:] = stats[
                    p * own_len : (p + 1) * own_len
                ].astype(BF16)

    vmem = pl.BlockSpec(memory_space=pltpu.VMEM)
    return pl.pallas_call(
        kernel,
        out_shape=jax.ShapeDtypeStruct((pairs, own_rows, lanes + head_dim), BF16),
        in_specs=[pl.BlockSpec(memory_space=pltpu.SMEM), vmem, vmem],
        out_specs=vmem,
        compiler_params=pltpu.CompilerParams(vmem_limit_bytes=WHOLE_VMEM),
        name="attend_part",
    )(where, swapped, spread)


def experts_forward(incoming, pieces):
    slots, width = incoming.shape
    counts = [piece.shape[0] for piece in pieces]
    offsets = [sum(counts[:n]) for n in range(len(pieces))]
    hidden_units = sum(counts)
    step_units = 256 if hidden_units % 256 == 0 else hidden_units

    def kernel(rows_ref, *refs):
        piece_refs = refs[: len(pieces)]
        out_ref, sum_ref, gate_ref, up_ref, down_ref, sems = refs[len(pieces) :]
        copies = [
            [
                pltpu.make_async_copy(
                    ref.at[:, pl.ds(n * width, width)],
                    target.at[pl.ds(offset, count), :],
                    sems.at[i * 3 + n],
                )
                for n, target in enumerate((gate_ref, up_ref, down_ref))
            ]
            for i, (ref, offset, count) in enumerate(zip(piece_refs, offsets, counts))
        ]
        for group in copies:
            for copy in group:
                copy.start()
        arrived = 0
        for low in range(0, hidden_units, step_units):
            while arrived < len(pieces) and offsets[arrived] < low + step_units:
                for copy in copies[arrived]:
                    copy.wait()
                arrived += 1
            span = slice(low, low + step_units)
            gate_part = dot(rows_ref[...], gate_ref[span, :], 1, 1)
            up_part = dot(rows_ref[...], up_ref[span, :], 1, 1)
            hidden = (gate_part / (1.0 + jnp.exp(-gate_part)) * up_part).astype(BF16)
            part = dot(hidden, down_ref[span, :], 1, 0)
            if low > 0:
                part = sum_ref[...] + part
            if low + step_units < hidden_units:
                sum_ref[...] = part
            else:
                out_ref[...] = part.astype(BF16)

    vmem = pl.BlockSpec(memory_space=pltpu.VMEM)
    return pl.pallas_call(
        kernel,
        out_shape=pltpu.VMEM((slots, width), BF16),
        in_specs=[vmem] + [pl.BlockSpec(memory_space=pltpu.HBM)] * len(pieces),
        out_specs=vmem,
        scratch_shapes=[pltpu.VMEM((slots, width), F32)]
        + [pltpu.VMEM((hidden_units, width), BF16)] * 3
        + [pltpu.SemaphoreType.DMA((3 * len(pieces),))],
        compiler_params=pltpu.CompilerParams(vmem_limit_bytes=24 << 20),
        name="experts_forward",
    )(pltpu.with_memory_space_constraint(incoming, pltpu.VMEM), *pieces)


def body(
    tokens_in,
    attn_gain,
    query_matrix,
    key_matrix,
    value_matrix,
    output_matrix,
    moe_gain,
    chosen_experts,
    combine_weights,
    gate_weight,
    up_weight,
    down_weight,
):
    pairs = lax.axis_size("pair")
    heads = lax.axis_size("head")
    blocks = lax.axis_size("ctx")
    seqs, own_len, width = tokens_in.shape
    own_rows = seqs * own_len
    rows = pairs * own_rows
    block_len = own_len * pairs
    q_cols = query_matrix.shape[1]
    part_cols = key_matrix.shape[0]
    head_dim = part_cols * pairs
    local_heads = q_cols // head_dim
    group = local_heads * pairs

    up_ring = [(i, (i + 1) % pairs) for i in range(pairs)]
    down_ring = [(i, (i - 1) % pairs) for i in range(pairs)]
    joined = jnp.concatenate([gate_weight[0], up_weight[0], down_weight[0]], axis=1)
    from_below = lax.ppermute(joined, "pair", up_ring)
    from_above = lax.ppermute(joined, "pair", down_ring)

    normed = normalize(tokens_in, attn_gain)
    token_send = for_each(normed, pairs)
    block_rows = exchange(token_send, "pair").reshape(rows, width)
    block_start = lax.axis_index("ctx") * block_len
    own_start = block_start + lax.axis_index("pair") * own_len
    places = jnp.arange(own_len)
    row_pos = block_start + (
        jnp.arange(pairs)[:, None, None] * own_len + jnp.zeros((seqs, 1), jnp.int32) + places
    ).reshape(rows)
    q_tables = rope_tables(row_pos.astype(F32), head_dim)
    key_value = dot(
        block_rows, jnp.concatenate([key_matrix, value_matrix], axis=0), 1, 1
    ).astype(BF16)
    query_raw = dot(block_rows, query_matrix, 1, 0)
    query = jnp.concatenate(
        [
            rotate(query_raw[:, j * head_dim : (j + 1) * head_dim], q_tables)
            for j in range(local_heads)
        ],
        axis=1,
    )
    swap_send = jnp.concatenate(
        [
            for_each(query, pairs),
            jnp.pad(
                key_value.reshape(pairs, own_rows, 2 * part_cols),
                ((0, 0), (0, 0), (0, q_cols - 2 * part_cols)),
            ),
        ],
        axis=1,
    )
    swapped = exchange(swap_send, "pair")
    own_pos = (own_start + jnp.zeros((seqs, 1), jnp.int32) + places).reshape(own_rows)
    key_own = jnp.concatenate([swapped[p, rows:, :part_cols] for p in range(pairs)], axis=1)
    value_own = jnp.concatenate(
        [swapped[p, rows:, part_cols : 2 * part_cols] for p in range(pairs)], axis=1
    )
    key_own = rotate(key_own.astype(F32), rope_tables(own_pos.astype(F32), head_dim))
    both = jnp.concatenate([key_own, value_own], axis=1)
    inner = math.isqrt(blocks)
    outer = blocks // inner
    near_groups = [[a * inner + b for b in range(inner)] for a in range(outer)]
    far_groups = [[a * inner + b for a in range(outer)] for b in range(inner)]
    kv_send = for_each(both, inner)
    near = exchange(kv_send, "ctx", near_groups)
    spread = exchange(for_each(near, outer).reshape(outer, -1, near.shape[-1]), "ctx", far_groups)
    spread = spread.reshape(blocks, own_rows, 2 * head_dim)

    head = lax.axis_index("head")
    group_cols = group * head_dim
    out_mine = lax.dynamic_slice_in_dim(output_matrix, head * group_cols, group_cols, 0)
    out_theirs = lax.dynamic_slice_in_dim(
        output_matrix, (heads - 1 - head) * group_cols, group_cols, 0
    )
    out_other = lax.ppermute(
        out_theirs, "head", [(h, heads - 1 - h) for h in range(heads)]
    )

    parts = attend_part(
        jnp.stack([block_start, lax.axis_index("pair")]).astype(jnp.int32),
        swapped,
        spread,
        seqs,
        own_len,
        local_heads,
        head_dim,
    )
    merged = exchange(parts, "pair")
    part_stats = (
        merged[..., group * head_dim : group * head_dim + group * 6]
        .astype(F32)
        .reshape(pairs, own_rows, group, 6)
    )
    part_peak = jnp.sum(part_stats[..., :3], axis=-1)
    part_total = jnp.sum(part_stats[..., 3:], axis=-1)
    scale = jnp.exp(part_peak - jnp.max(part_peak, axis=0))
    scale = scale / jnp.sum(scale * part_total, axis=0)
    part_mixed = merged[..., : group * head_dim].reshape(pairs, own_rows, group, head_dim)
    attended = jnp.sum(scale[..., None] * part_mixed.astype(F32), axis=0).astype(BF16)
    attended = attended.reshape(own_rows, group * head_dim)

    heads_send = for_each(attended, pairs)
    gathered_heads = exchange(heads_send, "pair").reshape(rows, group_cols)
    projected = jnp.stack(
        [dot(gathered_heads, out_mine, 1, 0), dot(gathered_heads, out_other, 1, 0)]
    ).astype(BF16)
    out_cols = output_matrix.shape[1]
    projected = (
        projected.reshape(2, pairs, seqs, own_len, out_cols)
        .transpose(2, 1, 0, 3, 4)
        .reshape(seqs * pairs, 2 * own_len, out_cols)
    )
    owned = exchange(projected, ("head", "pair"))
    owned = owned.reshape(heads, pairs, 2, own_len, out_cols).astype(F32)
    owned = (owned[:, :, 0] + owned[::-1, :, 1]).reshape(heads * pairs, own_len, out_cols)
    owned = jnp.moveaxis(owned, 0, 1).reshape(own_len, width)
    own_tokens = lax.dynamic_index_in_dim(tokens_in, lax.axis_index("head"), 0, keepdims=False)
    residual = (own_tokens.astype(F32) + rounded(owned)).astype(BF16)
    moe_in = normalize(residual, moe_gain)

    experts = blocks * heads
    top = chosen_experts.shape[-1]
    capacity = max(2, (own_len * top + experts - 1) // experts + 1)
    slots = experts * capacity
    picked = chosen_experts.reshape(own_len * top)
    earlier = jnp.tril(jnp.ones((own_len * top, own_len * top), jnp.bool_), -1)
    same = (picked[:, None] == picked[None, :]) & earlier
    slot_ids = picked * capacity + jnp.sum(same.astype(jnp.int32), axis=1)
    slot_ids = slot_ids.reshape(own_len, top)
    chosen_slot = slot_ids[..., None] == jnp.arange(slots)[None, None, :]
    placing = jnp.any(chosen_slot, axis=1).astype(BF16)
    outgoing = dot(placing, moe_in, 0, 0).astype(BF16)
    outgoing = outgoing.reshape(experts, capacity, width)
    incoming = exchange(outgoing, ("ctx", "head"))
    incoming = incoming.reshape(slots, width)

    half = joined.shape[0] // 2
    low_half = from_below[:half]
    high_half = from_above[half:]
    far_low = lax.ppermute(low_half, "pair", up_ring)
    far_high = lax.ppermute(high_half, "pair", down_ring)
    expert_out = experts_forward(incoming, [joined, from_below, from_above, far_low, far_high])
    returned = exchange(expert_out.reshape(experts, capacity, width), ("ctx", "head"))
    returned = returned.reshape(slots, width)
    share = jnp.sum(
        jnp.where(chosen_slot, combine_weights.reshape(own_len, top, 1), 0.0), axis=1
    )
    high = rounded(share)
    mixture = dot(jnp.concatenate([high, share - high], axis=0).astype(BF16), returned, 1, 0)
    mixture = mixture[:own_len] + mixture[own_len:]
    return (residual.astype(F32) + mixture).astype(BF16)[None]


def solution(mesh):
    return jax.shard_map(
        body,
        mesh=mesh,
        in_specs=(
            P(None, ("ctx", "pair"), None),
            P(),
            P(None, ("head", "pair")),
            P(("head", "pair"), None),
            P(("head", "pair"), None),
            P(None, ("head", "pair")),
            P(),
            P("head", ("ctx", "pair"), None),
            P("head", ("ctx", "pair"), None),
            P(("ctx", "head"), "pair", None),
            P(("ctx", "head"), "pair", None),
            P(("ctx", "head"), "pair", None),
        ),
        out_specs=P("head", ("ctx", "pair"), None),
        check_vma=False,
    )
```

```python
import jax
import jax.numpy as jnp
from jax import lax
from jax.experimental import pallas as pl
from jax.experimental.pallas import tpu as pltpu
from jax.sharding import PartitionSpec as P


ROPE_BASE = 1000000.0
EPSILON = 1e-06
MASKED = -1e30
F32 = jnp.float32
BF16 = jnp.bfloat16


def exchange(tiles, axis):
    return lax.all_to_all(tiles, axis, 0, 0, tiled=True)


def for_each(shard, count):
    return jnp.broadcast_to(shard[None], (count, *shard.shape))


def dot(a, b, a_dim, b_dim):
    return lax.dot_general(a, b, (((a_dim,), (b_dim,)), ((), ())), preferred_element_type=F32)


def normalize(values, gain_vector):
    wide = values.astype(F32)
    mean_square = jnp.mean(wide * wide, axis=-1, keepdims=True)
    return (wide * lax.rsqrt(mean_square + EPSILON) * gain_vector).astype(BF16)


def rope_tables(positions, head_dim):
    half_dim = head_dim // 2
    frequency = ROPE_BASE ** (-(jnp.arange(half_dim).astype(F32) * 2.0) / head_dim)
    angles = positions[:, None] * frequency[None, :]
    return jnp.cos(angles), jnp.sin(angles)


def rotate(values, tables):
    cosine_part, sine_part = tables
    half_dim = values.shape[-1] // 2
    lower_half = values[..., :half_dim]
    upper_half = values[..., half_dim:]
    return jnp.concatenate(
        [
            lower_half * cosine_part - upper_half * sine_part,
            upper_half * cosine_part + lower_half * sine_part,
        ],
        axis=-1,
    ).astype(BF16)


def rounded(values):
    return lax.reduce_precision(values, 8, 7)


STATS = 6
LOG2_E = 1.4426950408889634
GROUP_ROWS = 256
WHOLE_VMEM = 66_500_000


def attend_part(where, swapped, spread, seqs, own_len, local_heads, head_dim):
    pairs = swapped.shape[0]
    own_rows = seqs * own_len
    block_len = pairs * own_len
    blocks = spread.shape[0]
    group = pairs * local_heads
    lanes = group * head_dim
    scaling = head_dim ** (-0.5)
    heads_each = GROUP_ROWS // block_len

    def kernel(where_ref, swapped_ref, spread_ref, out_ref):
        start = where_ref[0]
        me = where_ref[1]
        key_index = lax.broadcasted_iota(jnp.int32, (1, blocks * own_len), 1)
        key_pos = (key_index // own_len) * block_len + me * own_len + key_index % own_len
        row = lax.broadcasted_iota(jnp.int32, (GROUP_ROWS, 1), 0)
        allowed = key_pos <= start + row % block_len
        lane = lax.broadcasted_iota(jnp.int32, (block_len, head_dim), 1)
        for seq in range(seqs):
            low = seq * own_len
            keys = spread_ref[:, low : low + own_len, :head_dim].reshape(-1, head_dim)
            values = spread_ref[:, low : low + own_len, head_dim:].reshape(-1, head_dim)
            stats = jnp.zeros((block_len, head_dim), F32)
            for first in range(0, group, heads_each):
                query = jnp.concatenate(
                    [
                        swapped_ref[
                            g // local_heads,
                            p * own_rows + low : p * own_rows + low + own_len,
                            (g % local_heads) * head_dim : (g % local_heads + 1) * head_dim,
                        ]
                        for g in range(first, first + heads_each)
                        for p in range(pairs)
                    ],
                    axis=0,
                )
                scores = jnp.where(allowed, dot(query, keys, 1, 1), MASKED)
                peak = jnp.maximum(jnp.max(scores, axis=1, keepdims=True), 0.1 * MASKED)
                probs = jnp.exp2((scores - peak) * (scaling * LOG2_E))
                total = jnp.sum(probs, axis=1, keepdims=True)
                mixed = dot(probs.astype(BF16), values, 1, 0).astype(BF16)
                terms = []
                for number in (peak * scaling, total):
                    high = number.astype(BF16).astype(F32)
                    middle = (number - high).astype(BF16).astype(F32)
                    terms += [high, middle, number - high - middle]
                for g in range(first, first + heads_each):
                    top = (g - first) * block_len
                    for p in range(pairs):
                        at = top + p * own_len
                        out_ref[
                            p, low : low + own_len, g * head_dim : (g + 1) * head_dim
                        ] = mixed[at : at + own_len]
                    for n, term in enumerate(terms):
                        stats = jnp.where(
                            lane == g * STATS + n, term[top : top + block_len], stats
                        )
            for p in range(pairs):
                out_ref[p, low : low + own_len, lanes:] = stats[
                    p * own_len : (p + 1) * own_len
                ].astype(BF16)

    vmem = pl.BlockSpec(memory_space=pltpu.VMEM)
    return pl.pallas_call(
        kernel,
        out_shape=jax.ShapeDtypeStruct((pairs, own_rows, lanes + head_dim), BF16),
        in_specs=[pl.BlockSpec(memory_space=pltpu.SMEM), vmem, vmem],
        out_specs=vmem,
        compiler_params=pltpu.CompilerParams(vmem_limit_bytes=WHOLE_VMEM),
        name="attend_part",
    )(where, swapped, spread)


def experts_forward(incoming, pieces):
    slots, width = incoming.shape
    counts = [piece.shape[0] for piece in pieces]
    offsets = [sum(counts[:n]) for n in range(len(pieces))]
    hidden_units = sum(counts)
    step_units = 256 if hidden_units % 256 == 0 else hidden_units

    def kernel(rows_ref, *refs):
        piece_refs = refs[: len(pieces)]
        out_ref, sum_ref, gate_ref, up_ref, down_ref, sems = refs[len(pieces) :]
        copies = [
            [
                pltpu.make_async_copy(
                    ref.at[:, pl.ds(n * width, width)],
                    target.at[pl.ds(offset, count), :],
                    sems.at[i * 3 + n],
                )
                for n, target in enumerate((gate_ref, up_ref, down_ref))
            ]
            for i, (ref, offset, count) in enumerate(zip(piece_refs, offsets, counts))
        ]
        for group in copies:
            for copy in group:
                copy.start()
        arrived = 0
        for low in range(0, hidden_units, step_units):
            while arrived < len(pieces) and offsets[arrived] < low + step_units:
                for copy in copies[arrived]:
                    copy.wait()
                arrived += 1
            span = slice(low, low + step_units)
            gate_part = dot(rows_ref[...], gate_ref[span, :], 1, 1)
            up_part = dot(rows_ref[...], up_ref[span, :], 1, 1)
            hidden = (gate_part / (1.0 + jnp.exp(-gate_part)) * up_part).astype(BF16)
            part = dot(hidden, down_ref[span, :], 1, 0)
            if low > 0:
                part = sum_ref[...] + part
            if low + step_units < hidden_units:
                sum_ref[...] = part
            else:
                out_ref[...] = part.astype(BF16)

    vmem = pl.BlockSpec(memory_space=pltpu.VMEM)
    return pl.pallas_call(
        kernel,
        out_shape=pltpu.VMEM((slots, width), BF16),
        in_specs=[vmem] + [pl.BlockSpec(memory_space=pltpu.HBM)] * len(pieces),
        out_specs=vmem,
        scratch_shapes=[pltpu.VMEM((slots, width), F32)]
        + [pltpu.VMEM((hidden_units, width), BF16)] * 3
        + [pltpu.SemaphoreType.DMA((3 * len(pieces),))],
        compiler_params=pltpu.CompilerParams(vmem_limit_bytes=24 << 20),
        name="experts_forward",
    )(pltpu.with_memory_space_constraint(incoming, pltpu.VMEM), *pieces)


def body(
    tokens_in,
    attn_gain,
    query_matrix,
    key_matrix,
    value_matrix,
    output_matrix,
    moe_gain,
    chosen_experts,
    combine_weights,
    gate_weight,
    up_weight,
    down_weight,
):
    pairs = lax.axis_size("pair")
    heads = lax.axis_size("head")
    blocks = lax.axis_size("ctx")
    seqs, own_len, width = tokens_in.shape
    own_rows = seqs * own_len
    rows = pairs * own_rows
    block_len = own_len * pairs
    q_cols = query_matrix.shape[1]
    part_cols = key_matrix.shape[0]
    head_dim = part_cols * pairs
    local_heads = q_cols // head_dim
    group = local_heads * pairs

    up_ring = [(i, (i + 1) % pairs) for i in range(pairs)]
    down_ring = [(i, (i - 1) % pairs) for i in range(pairs)]
    joined = jnp.concatenate([gate_weight[0], up_weight[0], down_weight[0]], axis=1)
    from_below = lax.ppermute(joined, "pair", up_ring)
    from_above = lax.ppermute(joined, "pair", down_ring)

    normed = normalize(tokens_in, attn_gain)
    token_send = for_each(normed, pairs)
    block_rows = exchange(token_send, "pair").reshape(rows, width)
    block_start = lax.axis_index("ctx") * block_len
    own_start = block_start + lax.axis_index("pair") * own_len
    places = jnp.arange(own_len)
    row_pos = block_start + (
        jnp.arange(pairs)[:, None, None] * own_len + jnp.zeros((seqs, 1), jnp.int32) + places
    ).reshape(rows)
    q_tables = rope_tables(row_pos.astype(F32), head_dim)
    key_value = dot(
        block_rows, jnp.concatenate([key_matrix, value_matrix], axis=0), 1, 1
    ).astype(BF16)
    query_raw = dot(block_rows, query_matrix, 1, 0)
    query = jnp.concatenate(
        [
            rotate(query_raw[:, j * head_dim : (j + 1) * head_dim], q_tables)
            for j in range(local_heads)
        ],
        axis=1,
    )
    swap_send = jnp.concatenate(
        [
            for_each(query, pairs),
            jnp.pad(
                key_value.reshape(pairs, own_rows, 2 * part_cols),
                ((0, 0), (0, 0), (0, q_cols - 2 * part_cols)),
            ),
        ],
        axis=1,
    )
    swapped = exchange(swap_send, "pair")
    own_pos = (own_start + jnp.zeros((seqs, 1), jnp.int32) + places).reshape(own_rows)
    key_own = jnp.concatenate([swapped[p, rows:, :part_cols] for p in range(pairs)], axis=1)
    value_own = jnp.concatenate(
        [swapped[p, rows:, part_cols : 2 * part_cols] for p in range(pairs)], axis=1
    )
    key_own = rotate(key_own.astype(F32), rope_tables(own_pos.astype(F32), head_dim))
    both = jnp.concatenate([key_own, value_own], axis=1)
    kv_send = for_each(both, blocks)
    spread = exchange(kv_send, "ctx")

    head = lax.axis_index("head")
    group_cols = group * head_dim
    out_mine = lax.dynamic_slice_in_dim(output_matrix, head * group_cols, group_cols, 0)
    out_theirs = lax.dynamic_slice_in_dim(
        output_matrix, (heads - 1 - head) * group_cols, group_cols, 0
    )
    out_other = lax.ppermute(
        out_theirs, "head", [(h, heads - 1 - h) for h in range(heads)]
    )

    parts = attend_part(
        jnp.stack([block_start, lax.axis_index("pair")]).astype(jnp.int32),
        swapped,
        spread,
        seqs,
        own_len,
        local_heads,
        head_dim,
    )
    merged = exchange(parts, "pair")
    part_stats = (
        merged[..., group * head_dim : group * head_dim + group * 6]
        .astype(F32)
        .reshape(pairs, own_rows, group, 6)
    )
    part_peak = jnp.sum(part_stats[..., :3], axis=-1)
    part_total = jnp.sum(part_stats[..., 3:], axis=-1)
    scale = jnp.exp(part_peak - jnp.max(part_peak, axis=0))
    scale = scale / jnp.sum(scale * part_total, axis=0)
    part_mixed = merged[..., : group * head_dim].reshape(pairs, own_rows, group, head_dim)
    attended = jnp.sum(scale[..., None] * part_mixed.astype(F32), axis=0).astype(BF16)
    attended = attended.reshape(own_rows, group * head_dim)

    heads_send = for_each(attended, pairs)
    gathered_heads = exchange(heads_send, "pair").reshape(rows, group_cols)
    projected = jnp.stack(
        [dot(gathered_heads, out_mine, 1, 0), dot(gathered_heads, out_other, 1, 0)]
    ).astype(BF16)
    out_cols = output_matrix.shape[1]
    projected = (
        projected.reshape(2, pairs, seqs, own_len, out_cols)
        .transpose(2, 1, 0, 3, 4)
        .reshape(seqs * pairs, 2 * own_len, out_cols)
    )
    owned = exchange(projected, ("head", "pair"))
    owned = owned.reshape(heads, pairs, 2, own_len, out_cols).astype(F32)
    owned = (owned[:, :, 0] + owned[::-1, :, 1]).reshape(heads * pairs, own_len, out_cols)
    owned = jnp.moveaxis(owned, 0, 1).reshape(own_len, width)
    own_tokens = lax.dynamic_index_in_dim(tokens_in, lax.axis_index("head"), 0, keepdims=False)
    residual = (own_tokens.astype(F32) + rounded(owned)).astype(BF16)
    moe_in = normalize(residual, moe_gain)

    experts = blocks * heads
    top = chosen_experts.shape[-1]
    capacity = max(2, (own_len * top + experts - 1) // experts + 1)
    slots = experts * capacity
    picked = chosen_experts.reshape(own_len * top)
    earlier = jnp.tril(jnp.ones((own_len * top, own_len * top), jnp.bool_), -1)
    same = (picked[:, None] == picked[None, :]) & earlier
    slot_ids = picked * capacity + jnp.sum(same.astype(jnp.int32), axis=1)
    slot_ids = slot_ids.reshape(own_len, top)
    chosen_slot = slot_ids[..., None] == jnp.arange(slots)[None, None, :]
    placing = jnp.any(chosen_slot, axis=1).astype(BF16)
    outgoing = dot(placing, moe_in, 0, 0).astype(BF16)
    outgoing = outgoing.reshape(experts, capacity, width)
    incoming = exchange(outgoing, ("ctx", "head"))
    incoming = incoming.reshape(slots, width)

    half = joined.shape[0] // 2
    low_half = from_below[:half]
    high_half = from_above[half:]
    far_low = lax.ppermute(low_half, "pair", up_ring)
    far_high = lax.ppermute(high_half, "pair", down_ring)
    expert_out = experts_forward(incoming, [joined, from_below, from_above, far_low, far_high])
    returned = exchange(expert_out.reshape(experts, capacity, width), ("ctx", "head"))
    returned = returned.reshape(slots, width)
    share = jnp.sum(
        jnp.where(chosen_slot, combine_weights.reshape(own_len, top, 1), 0.0), axis=1
    )
    high = rounded(share)
    mixture = dot(jnp.concatenate([high, share - high], axis=0).astype(BF16), returned, 1, 0)
    mixture = mixture[:own_len] + mixture[own_len:]
    return (residual.astype(F32) + mixture).astype(BF16)[None]


def solution(mesh):
    return jax.shard_map(
        body,
        mesh=mesh,
        in_specs=(
            P(None, ("ctx", "pair"), None),
            P(),
            P(None, ("head", "pair")),
            P(("head", "pair"), None),
            P(("head", "pair"), None),
            P(None, ("head", "pair")),
            P(),
            P("head", ("ctx", "pair"), None),
            P("head", ("ctx", "pair"), None),
            P(("ctx", "head"), "pair", None),
            P(("ctx", "head"), "pair", None),
            P(("ctx", "head"), "pair", None),
        ),
        out_specs=P("head", ("ctx", "pair"), None),
        check_vma=False,
    )
```
